32 devices in a mesh: seq: 16 (over z, x, core), mp: 2 (over y).
Axes of the slice: x: 2, y: 2, z: 4, core: 2. Of those that a mesh axis runs over, the one named last changes fastest.
Arguments:
- x_inner: bfloat16 [2, 4096, 5120], P(None, 'seq', 'mp'), may hold values from -6 to 6
- z_gate: bfloat16 [2, 4096, 5120], P(None, 'seq', 'mp'), may hold values from -6 to 6
- b_input: bfloat16 [2, 4096, 128], P(None, 'seq'), may hold values from -6 to 6
- c_input: bfloat16 [2, 4096, 128], P(None, 'seq'), may hold values from -6 to 6
- dt_raw: float32 [2, 4096, 80], P(None, 'seq', 'mp'), may hold values from -3 to 3
- doc_ids: int32 [2, 4096], P(None, 'seq'), may hold values from 0 to 2, never falling along the last dimension, each value on 1 to 2048 neighbouring positions
- conv_x: bfloat16 [4, 5120], P(None, 'mp'), may hold values from -3 to 3
- conv_b: bfloat16 [4, 128], replicated, may hold values from -3 to 3
- conv_c: bfloat16 [4, 128], replicated, may hold values from -3 to 3
- dt_bias: float32 [80], P('mp'), as said below
- decay_rate: float32 [80], P('mp'), may hold values from 0.0625 to 0.25
- norm_gain: float32 [5120], P('mp'), may hold values from 0.25 to 1.75
- w_out: bfloat16 [5120, 2560], P('mp'), may hold values from -0.078125 to 0.078125
Outputs:
- layer_out: bfloat16 [2, 4096, 2560], P(None, 'seq', 'mp')
The draws below stay inside these ranges and needn't reach their ends.
Inputs may be any that keep to these rules, and one draw needn't show every extreme that they name: `doc_ids`: in each sequence the document numbers start at 0, never fall and rise by one at each new document; there are three documents, the longest exactly 2048 positions. `dt_bias`: softplus of each entry lies between 8/4096 and 1.
All inputs are finite; a program needn't handle non-finite values.
Results may differ from the reference program's by a relative error of at most 0.02.
Values may be sent and summed in bfloat16 or wider, within the bound.
A program may use at most 128 MiB of HBM per device.

```python
import math
import jax
import jax.numpy as jnp
import numpy as np
from jax import lax

D = 2560
HEADS = 80
HEADDIM = 64
DSTATE = 128
CONV = 4
BLOCK = 256
BATCH = 2
SEQLEN = 4096
INNER = 5120
N_MP = 2


def draw_dt_bias(key, part):
    level = jax.random.uniform(key, (HEADS,), jnp.float32)
    lowest = jnp.log(8.0 / SEQLEN)
    target = jnp.exp(lowest * level)
    return jnp.log(jnp.expm1(target)).astype(jnp.float32)


def levels(stream_key, shape, pieces, low, largest):
    def one(axis_at, parts):
        draws = jax.random.uniform(jax.random.fold_in(jax.random.fold_in(stream_key, 6), axis_at), (parts,), jnp.float32, low / len(pieces), largest / len(pieces))
        return jnp.repeat(jnp.exp(draws), shape[axis_at] // parts).reshape((-1,) + (1,) * (len(shape) - axis_at - 1))

    loudness = one(*pieces[0])
    for cut in pieces[1:]:
        loudness = loudness * one(*cut)
    return loudness


def split_up(amount, total, limit, slope):
    weights = [(1 << 20) // math.isqrt(rank ** slope) + 1 for rank in range(2, amount + 1)]
    surplus, holding = total - limit - (amount - 1), [1] * (amount - 1)
    while surplus > 0:
        movable = [i for i in range(amount - 1) if holding[i] < limit]
        whole, remaining = sum([weights[i] for i in movable]), surplus
        for i in movable:
            more = min(limit - holding[i], max(1, remaining * weights[i] // whole), surplus)
            holding[i] = holding[i] + more
            surplus = surplus - more
    return np.array([limit] + holding)


def ragged_sizes(rng, number_of, total, reach, skew):
    if number_of == 2:
        one = jax.random.randint(rng, (), max(1, total - reach), min(reach, total - 1) + 1)
        return jnp.stack([one, total - one])
    tallies = jnp.asarray(split_up(number_of, total, reach, skew), jnp.int32)
    twos = (number_of - 1) // 2
    source_of, sink = tallies[1:1 + 2 * twos:2], tallies[2:2 + 2 * twos:2]
    slack = jnp.minimum(source_of - 1, reach - sink)
    passed = jax.random.randint(jax.random.fold_in(rng, 1), (twos,), 0, 1 << 20) % (slack + 1)
    tallies = tallies.at[1:1 + 2 * twos:2].set(source_of - passed).at[2:2 + 2 * twos:2].set(sink + passed)
    return tallies[jax.random.permutation(jax.random.fold_in(rng, 2), number_of)]


def scatter_about(stream_key, extent, deviation, bound, shards=(), held_as=jnp.bfloat16):
    gain = levels(stream_key, extent, shards, -0.22, 0.18) if shards else 1.0
    values = jax.random.normal(stream_key, extent, jnp.float32) * deviation * gain
    return jnp.minimum(jnp.maximum(values, -bound), bound).astype(held_as)


def setup_inputs(seed: int = 0) -> dict:
    streams_of = jax.random.split(jax.random.key(seed), 14)
    x_inner = scatter_about(streams_of[0], (BATCH, SEQLEN, INNER), 1.0, 6.0, ((1, 16), (2, 2)))
    z_gate = scatter_about(streams_of[1], (BATCH, SEQLEN, INNER), 1.0, 6.0, ((1, 16), (2, 2)))
    b_input = scatter_about(streams_of[2], (BATCH, SEQLEN, DSTATE), 1.0, 6.0, ((1, 16),))
    c_input = scatter_about(streams_of[3], (BATCH, SEQLEN, DSTATE), 1.0, 6.0, ((1, 16),))
    dt_raw = scatter_about(streams_of[4], (BATCH, SEQLEN, HEADS), 0.5, 3.0, ((1, 16), (2, 2)), jnp.float32)
    doc_ids = jax.vmap(lambda own: jnp.searchsorted(jnp.cumsum(ragged_sizes(own, 3, SEQLEN, SEQLEN // 2, 0)), jnp.arange(SEQLEN), side="right"))(jax.random.split(streams_of[5], BATCH)).reshape((BATCH, SEQLEN)).astype(jnp.int32)
    conv_x = scatter_about(streams_of[6], (CONV, INNER), CONV ** -0.5, 3.0, ((1, 2),))
    conv_b = scatter_about(streams_of[7], (CONV, DSTATE), CONV ** -0.5, 3.0)
    conv_c = scatter_about(streams_of[8], (CONV, DSTATE), CONV ** -0.5, 3.0)
    dt_bias = draw_dt_bias(jax.random.fold_in(streams_of[13], 71), 0)
    decay_rate = jnp.clip(jnp.exp(math.log(0.25) - 1.3862944 * jax.random.uniform(streams_of[10], (HEADS,), jnp.float32) ** levels(streams_of[10], (HEADS,), ((0, 2),), -0.2, 0.2)), 0.0625, 0.25)
    norm_gain = jnp.clip(1.0 + 0.15 * jax.random.normal(streams_of[11], (INNER,), jnp.float32), 0.25, 1.75)
    w_out = scatter_about(streams_of[12], (INNER, D), INNER ** -0.5, 0.078125, ((0, 2),))
    return {"x_inner": x_inner, "z_gate": z_gate, "b_input": b_input, "c_input": c_input, "dt_raw": dt_raw, "doc_ids": doc_ids, "conv_x": conv_x, "conv_b": conv_b, "conv_c": conv_c, "dt_bias": dt_bias, "decay_rate": decay_rate, "norm_gain": norm_gain, "w_out": w_out}


EPSILON = 1e-05

def causal_conv(values, docs, weight):
    taps = weight.shape[0]
    length = values.shape[0]
    window = jnp.concatenate([jnp.zeros((taps - 1, values.shape[1]), jnp.bfloat16), values], axis=0)
    marks = jnp.concatenate([jnp.full((taps - 1,), -1, jnp.int32), docs.astype(jnp.int32)], axis=0)
    total = jnp.zeros(values.shape, jnp.float32)
    for offset in range(taps):
        same = (marks[offset:offset + length] == docs)[:, None]
        term = window[offset:offset + length].astype(jnp.float32) * weight[offset].astype(jnp.float32)
        total = total + jnp.where(same, term, 0.0)
    return jax.nn.silu(total).astype(jnp.bfloat16)

def sequence_mix(xs, bs, cs, steps, docs, rates):
    blocks = SEQLEN // BLOCK
    xs_b = xs.reshape(blocks, BLOCK, HEADS, HEADDIM)
    bs_b = bs.reshape(blocks, BLOCK, DSTATE)
    cs_b = cs.reshape(blocks, BLOCK, DSTATE)
    steps_b = steps.reshape(blocks, BLOCK, HEADS)
    docs_b = docs.reshape(blocks, BLOCK)
    order = jnp.arange(BLOCK)
    causal = order[:, None] >= order[None, :]

    def step_block(carry, block):
        state, before = carry
        xs_c, bs_c, cs_c, steps_c, docs_c = block
        logs = jnp.cumsum(-(steps_c * rates), axis=0)
        masked = causal & (docs_c[:, None] == docs_c[None, :])
        scores = jnp.dot(cs_c, bs_c.T, preferred_element_type=jnp.float32)
        spread = jnp.where(masked[:, :, None], logs[:, None, :] - logs[None, :, :], 0.0)
        mixing = jnp.where(masked[:, :, None], scores[:, :, None] * jnp.exp(spread) * steps_c[None, :, :], 0.0).astype(jnp.bfloat16)
        inner = jnp.einsum('tsh,shp->thp', mixing.astype(jnp.float32), xs_c.astype(jnp.float32))
        keeps = (docs_c == docs_c[-1])[:, None]
        weights = jnp.where(keeps, jnp.exp(logs[-1:] - logs) * steps_c, 0.0)
        loaded = (weights[:, :, None] * bs_c[:, None, :].astype(jnp.float32)).astype(jnp.bfloat16)
        fresh = jnp.einsum('shp,shn->hpn', xs_c.astype(jnp.float32), loaded.astype(jnp.float32))
        carried = docs_c == before
        entry = jnp.where(carried[:, None], jnp.exp(logs), 0.0)
        entering = state.astype(jnp.bfloat16)
        outer = jnp.einsum('tn,hpn->thp', cs_c.astype(jnp.float32), entering.astype(jnp.float32))
        mixed = inner + entry[:, :, None] * outer
        new_state = entry[-1][:, None, None] * state + fresh
        return ((new_state, docs_c[-1]), mixed)
    start = (jnp.zeros((HEADS, HEADDIM, DSTATE), jnp.float32), jnp.array(-1, dtype=jnp.int32))
    final, mixed_all = lax.scan(step_block, start, (xs_b, bs_b, cs_b, steps_b, docs_b))
    return mixed_all.reshape(SEQLEN, INNER)

def reference(x_inner, z_gate, b_input, c_input, dt_raw, doc_ids, conv_x, conv_b, conv_c, dt_bias, decay_rate, norm_gain, w_out):
    group = INNER // N_MP
    results = []
    for member in range(BATCH):
        docs = doc_ids[member].astype(jnp.int32)
        xs = causal_conv(x_inner[member], docs, conv_x)
        bs = causal_conv(b_input[member], docs, conv_b)
        cs = causal_conv(c_input[member], docs, conv_c)
        steps = jax.nn.softplus(dt_raw[member] + dt_bias)
        mixed = sequence_mix(xs.reshape(SEQLEN, HEADS, HEADDIM), bs, cs, steps, docs, decay_rate)
        gated = mixed * jax.nn.silu(z_gate[member].astype(jnp.float32))
        scale = lax.rsqrt(lax.optimization_barrier(jnp.sum(gated * gated, axis=1)) / INNER + EPSILON)
        normed = (gated * scale[:, None] * norm_gain).astype(jnp.bfloat16)
        total = jnp.zeros((SEQLEN, D), jnp.float32)
        for member_group in range(N_MP):
            lower = member_group * group
            partial_value = jnp.dot(normed[:, lower:lower + group], w_out[lower:lower + group], preferred_element_type=jnp.float32).astype(jnp.bfloat16)
            total = total + lax.optimization_barrier(partial_value).astype(jnp.float32)
        results.append(total.astype(jnp.bfloat16))
    return jnp.stack(results, axis=0)
```

```python
import functools

import jax
import jax.numpy as jnp
from jax import lax
from jax.experimental import pallas as pl
from jax.experimental.pallas import tpu as pltpu
from jax.sharding import PartitionSpec as P

EPSILON = 1e-05
LANES = 128
EDGE = 16
LOG2E = 1.4426950408889634
CAP = 80.0
MESH = pl.DeviceIdType.MESH
F32 = jnp.float32
BF16 = jnp.bfloat16


def silu(value):
    half = 0.5 * value
    return half + half * jnp.tanh(half)


def wide(value, width):
    return value if width == LANES else jnp.concatenate([value] * (width // LANES), axis=1)


def kernel(
    dims,
    x_ref,
    z_hbm,
    b_ref,
    c_ref,
    dt_ref,
    doc_ref,
    wx_ref,
    wb_ref,
    wc_ref,
    bias_ref,
    rate_ref,
    gain_ref,
    w_hbm,
    out_ref,
    z_ref,
    w_ref,
    hx_ref,
    hb_ref,
    hc_ref,
    hd_ref,
    same_ref,
    xc_ref,
    cc_ref,
    bt_ref,
    score_ref,
    col_ref,
    load_ref,
    entry_ref,
    row_ref,
    pad_ref,
    s_ref,
    r_ref,
    g_ref,
    gr_ref,
    e_ref,
    o_ref,
    t_ref,
    en_ref,
    inner_ref,
    gn_ref,
    p_ref,
    q_ref,
    own_ref,
    sq_ref,
    sqr_ref,
    z_sem,
    w_sem,
    halo_send,
    halo_recv,
    s_send,
    s_recv,
    g_send,
    g_recv,
    e_send,
    e_recv,
    t_send,
    t_recv,
    p_send,
    p_recv,
    sq_send,
    sq_recv,
):
    batch, length, channels, heads, width, piece, aligned, n_mp = dims
    inner_total = channels * n_mp
    head_dim = channels // heads
    cw = 2 * LANES if channels % (2 * LANES) == 0 else LANES
    per_tile = LANES // head_dim
    per_chunk = cw // head_dim
    chunks = channels // cw
    units = batch * chunks
    steps = units // 2
    pieces = width // piece
    n_seq = lax.axis_size("seq")
    me = lax.axis_index("seq")
    my = lax.axis_index("mp")
    core = lax.rem(me, 2)
    sibling = me + 1 - 2 * core

    def blocks(k):
        if aligned:
            return w_hbm.at[:, pl.ds(pl.multiple_of(k * piece, piece), piece)]
        return w_hbm.at[k]

    barrier = pltpu.get_barrier_semaphore()
    expected = jnp.int32(n_mp - 1)
    for distance in (-2, -1, 1, 2):
        there = me + distance
        valid = jnp.logical_and(there >= 0, there < n_seq)
        expected = expected + valid.astype(jnp.int32)

        @pl.when(valid)
        def _(there=there):
            pl.semaphore_signal(barrier, inc=1, device_id={"seq": there}, device_id_type=MESH)

    for r in range(1, n_mp):
        pl.semaphore_signal(
            barrier, inc=1, device_id={"mp": lax.rem(my + r, n_mp)}, device_id_type=MESH
        )
    z_copy = pltpu.make_async_copy(z_hbm, z_ref, z_sem)
    z_copy.start()

    def w_copy(k):
        return pltpu.make_async_copy(blocks(k), w_ref.at[k], w_sem.at[k])

    def w_start(k, _):
        w_copy(k).start()
        return 0

    pl.semaphore_wait(barrier, expected)

    def remote(src, dst, send, recv, **there):
        return pltpu.make_async_remote_copy(
            src_ref=src,
            dst_ref=dst,
            send_sem=send,
            recv_sem=recv,
            device_id=there,
            device_id_type=MESH,
        )

    right = lax.rem(me + 1, n_seq)
    last = pl.ds(length - EDGE, EDGE)
    halos = [
        remote(doc_ref, hd_ref, halo_send.at[0], halo_recv.at[0], seq=right),
        remote(b_ref.at[:, last], hb_ref, halo_send.at[1], halo_recv.at[1], seq=right),
        remote(c_ref.at[:, last], hc_ref, halo_send.at[2], halo_recv.at[2], seq=right),
        remote(x_ref.at[:, last], hx_ref, halo_send.at[3], halo_recv.at[3], seq=right),
    ]

    @pl.when(me < n_seq - 1)
    def _():
        for halo in halos:
            halo.start()

    lax.fori_loop(0, n_mp * pieces, w_start, 0)

    @pl.when(me == 0)
    def _():
        hd_ref[...] = jnp.full_like(hd_ref, -1.0)
        hb_ref[...] = jnp.zeros_like(hb_ref)
        hc_ref[...] = jnp.zeros_like(hc_ref)
        hx_ref[...] = jnp.zeros_like(hx_ref)

    @pl.when(me < 2)
    def _():
        e_ref[...] = jnp.zeros_like(e_ref)

    rows = lax.broadcasted_iota(jnp.int32, (length, length), 0)
    columns = lax.broadcasted_iota(jnp.int32, (length, length), 1)
    causal = rows >= columns
    triangle = jnp.where(causal, 1.0, 0.0).astype(F32)
    lane_ids = lax.broadcasted_iota(jnp.int32, (length, LANES), 1)

    for b in range(batch):
        step = dt_ref[b] + bias_ref[...]
        step = jnp.maximum(step, 0.0) + jnp.log1p(jnp.exp(-jnp.abs(step)))
        pad_ref[b] = jnp.zeros((length, LANES), F32)
        pad_ref[batch + b] = jnp.ones((length, LANES), F32)
        pad_ref[b, :, 0:heads] = -(step * rate_ref[...])
        pad_ref[batch + b, :, 0:heads] = step
        logs = jnp.dot(
            triangle, pad_ref[b], precision=lax.Precision.HIGHEST, preferred_element_type=F32
        )
        col_ref[b] = logs * LOG2E
        row_ref[b] = (logs * LOG2E - jnp.log(pad_ref[batch + b]) * LOG2E).T

    @pl.when(me > 0)
    def _():
        for halo in halos:
            halo.wait_recv()

    def conv(now, halo, weight, same):
        full = jnp.concatenate([halo.astype(F32), now.astype(F32)], axis=0)
        taps = weight.shape[0]
        weight = weight.astype(F32)
        total = full[EDGE:] * weight[taps - 1 : taps]
        for lag in range(1, taps):
            shifted = pltpu.roll(full, lag, 0)[EDGE:]
            total = total + shifted * same[lag - 1] * weight[taps - 1 - lag : taps - lag]
        return silu(total)

    for b in range(batch):
        doc_row = doc_ref[b, 0:1, :]
        doc_col = jnp.broadcast_to(doc_row, (LANES, length)).T
        old_col = jnp.broadcast_to(hd_ref[b, 0:1, :], (LANES, length)).T
        full = jnp.concatenate([old_col[length - EDGE :], doc_col], axis=0)
        for lag in range(1, wx_ref.shape[0]):
            mark = pltpu.roll(full, lag, 0)[EDGE:]
            same = jnp.where(mark == doc_col, 1.0, 0.0).astype(F32)
            same_ref[b, lag - 1] = wide(same, cw)
        sames = [same_ref[b, lag, :, 0:LANES] for lag in range(wx_ref.shape[0] - 1)]
        b_conv = conv(b_ref[b], hb_ref[b], wb_ref[...], sames).astype(BF16)
        c_conv = conv(c_ref[b], hc_ref[b], wc_ref[...], sames).astype(BF16)
        cc_ref[b] = c_conv
        bt = b_conv.astype(F32).T.astype(BF16)
        bt_ref[b] = bt
        scores = jnp.dot(c_conv, bt, preferred_element_type=F32)
        masked = jnp.logical_and(causal, wide(doc_col, length) == doc_row)
        score_ref[b] = jnp.where(masked, scores, 0.0)
        logs = col_ref[b]
        step = pad_ref[batch + b]
        keeps = doc_col == doc_col[length - 1 : length]
        load_ref[b] = jnp.where(keeps, jnp.exp2(logs[length - 1 : length] - logs) * step, 0.0)
        before = old_col[length - 1 : length]
        entry_ref[b] = jnp.where(doc_col == before, jnp.exp2(logs), 0.0)

    def place(u):
        b = u // chunks
        c = u - b * chunks
        return b, c, pl.ds(pl.multiple_of(c * cw, cw), cw)

    def turned(value, c):
        return pltpu.roll(value, lax.rem(LANES - c * per_chunk, LANES), 1)

    def expand(value):
        ids = lax.broadcasted_iota(jnp.int32, (value.shape[0], LANES), 1)
        parts = []
        for tile in range(cw // LANES):
            first = tile * per_tile
            part = value[:, first : first + 1]
            for more in range(1, per_tile):
                column = value[:, first + more : first + more + 1]
                part = jnp.where(ids < more * head_dim, part, column)
            parts.append(jnp.broadcast_to(part, (value.shape[0], LANES)))
        return jnp.concatenate(parts, axis=1) if len(parts) > 1 else parts[0]

    def s_copy(u):
        return remote(
            s_ref.at[u], r_ref.at[u // 2], s_send.at[u // 2], s_recv.at[u // 2], seq=sibling
        )

    def front(u, _):
        b, c, where = place(u)
        sames = [same_ref[b, lag] for lag in range(wx_ref.shape[0] - 1)]
        x_conv = conv(x_ref[b, :, where], hx_ref[b, :, where], wx_ref[:, where], sames)
        x_conv = x_conv.astype(BF16)
        xc_ref[b, :, where] = x_conv
        weights = expand(turned(load_ref[b], c))
        weighted = (x_conv.astype(F32) * weights).astype(BF16)
        s_ref[u] = jnp.dot(bt_ref[b], weighted, preferred_element_type=F32).astype(BF16)
        gate = expand(turned(entry_ref[b, length - 8 : length, :], c))
        g_ref[u] = jnp.broadcast_to(gate[7:8], (8, cw))

        @pl.when(lax.rem(u, 2) != core)
        def _():
            s_copy(u).start()

        return 0

    lax.fori_loop(0, units, front, 0)
    g_copy = remote(g_ref, gr_ref, g_send, g_recv, seq=sibling)
    g_copy.start()
    g_copy.wait_recv()
    ahead = lax.rem(me + 2, n_seq)

    def e_copy(i):
        return remote(o_ref.at[i], e_ref.at[i], e_send.at[i], e_recv.at[i], seq=ahead)

    def t_copy(i, owner):
        u = 2 * i + owner
        return remote(t_ref.at[i], en_ref.at[u], t_send.at[i], t_recv.at[i], seq=sibling)

    def inner_unit(u):
        b, c, where = place(u)
        turned_logs = turned(col_ref[b], c)
        scores = score_ref[b]
        for tile in range(cw // LANES):
            lanes = pl.ds(pl.multiple_of(c * cw + tile * LANES, LANES), LANES)
            xs = xc_ref[b, :, lanes]
            total = None
            for more in range(per_tile):
                head = tile * per_tile + more
                column = turned_logs[:, head : head + 1]
                row = row_ref[b, pl.ds(c * per_chunk + head, 1), :]
                mixing = scores * jnp.exp2(jnp.minimum(column - row, CAP))
                one = jnp.dot(mixing.astype(BF16), xs, preferred_element_type=F32)
                total = one if more == 0 else jnp.where(lane_ids < more * head_dim, total, one)
            inner_ref[b, :, lanes] = total

    def chain(i, _):
        u = 2 * i + core
        s_copy(2 * i).wait_recv()
        mine, theirs = s_ref[u].astype(F32), r_ref[i].astype(F32)
        my_gate, their_gate = g_ref[u, 0:1, :], gr_ref[u, 0:1, :]
        first = core == 0
        state_a = jnp.where(first, mine, theirs)
        state_b = jnp.where(first, theirs, mine)
        gate_a = jnp.where(first, my_gate, their_gate)
        gate_b = jnp.where(first, their_gate, my_gate)

        @pl.when(me >= 2)
        def _():
            e_copy(i).wait_recv()

        entering = e_ref[i].astype(F32)
        middle = gate_a * entering + state_a
        o_ref[i] = (gate_b * middle + state_b).astype(BF16)

        @pl.when(me + 2 < n_seq)
        def _():
            e_copy(i).start()

        t_ref[i] = jnp.where(first, middle, entering).astype(BF16)
        t_copy(i, core).start()
        en_ref[u] = jnp.where(first, entering, middle).astype(BF16)
        inner_unit(2 * i)
        inner_unit(2 * i + 1)
        return 0

    def t_wait(i, _):
        t_copy(i, 1 - core).wait_recv()
        return 0

    def p_slot(b, r, p):
        return (b * (n_mp - 1) + r - 1) * pieces + p

    def p_copy(b, r, p):
        slot = p_slot(b, r, p)
        return remote(
            p_ref.at[slot],
            q_ref.at[slot],
            p_send.at[slot],
            p_recv.at[slot],
            mp=lax.rem(my + r, n_mp),
        )

    def sq_copy(b, r):
        slot = b * (n_mp - 1) + r - 1
        return remote(
            sq_ref.at[b],
            sqr_ref.at[slot],
            sq_send.at[slot],
            sq_recv.at[slot],
            mp=lax.rem(my + r, n_mp),
        )

    def tail(b):
        def gate_unit(c, squares):
            where = pl.ds(pl.multiple_of(c * cw, cw), cw)
            outer = jnp.dot(cc_ref[b], en_ref[b * chunks + c], preferred_element_type=F32)
            mixed = inner_ref[b, :, where] + expand(turned(entry_ref[b], c)) * outer
            gated = mixed * silu(z_ref[b, :, where].astype(F32))
            gn_ref[:, where] = (gated * gain_ref[0:1, where]).astype(BF16)
            square = gated * gated
            for tile in range(cw // LANES):
                squares = squares + square[:, tile * LANES : (tile + 1) * LANES]
            return squares

        squares = lax.fori_loop(0, chunks, gate_unit, jnp.zeros((length, LANES), F32))
        sq_ref[b] = jnp.broadcast_to(jnp.sum(squares.T, axis=0, keepdims=True), (8, length))
        for r in range(1, n_mp):

            def project(p, _, r=r):
                k = lax.rem(my + r, n_mp) * pieces + p
                value = jnp.dot(gn_ref[...], w_ref[k], preferred_element_type=F32)
                p_ref[p_slot(b, r, p)] = value.astype(BF16)
                p_copy(b, r, p).start()
                return 0

            sq_copy(b, r).start()
            lax.fori_loop(0, pieces, project, 0)

        def project_own(p, _):
            value = jnp.dot(gn_ref[...], w_ref[my * pieces + p], preferred_element_type=F32)
            own_ref[b * pieces + p] = value
            return 0

        lax.fori_loop(0, pieces, project_own, 0)

    def finish(b):
        total = sq_ref[b]
        for r in range(1, n_mp):
            sq_copy(b, r).wait_recv()
            total = total + sqr_ref[b * (n_mp - 1) + r - 1]
        scale = lax.rsqrt(total[0:1] / inner_total + EPSILON)
        scale = jnp.broadcast_to(scale, (LANES, length)).T[:, 0:1]
        for p in range(pieces):
            value = own_ref[b * pieces + p]
            for r in range(1, n_mp):
                p_copy(b, r, p).wait_recv()
                value = value + q_ref[p_slot(b, r, p)].astype(F32)
            out_ref[b, :, p * piece : (p + 1) * piece] = (value * scale).astype(BF16)

    lower = 0
    for b in range(batch):
        upper = ((b + 1) * chunks + 1) // 2
        lax.fori_loop(lower, upper, chain, 0)
        lax.fori_loop(lower, upper, t_wait, 0)
        if b == 0:
            z_copy.wait()
            lax.fori_loop(0, n_mp * pieces, lambda k, _: (w_copy(k).wait(), 0)[1], 0)
        tail(b)
        lower = upper
    for b in range(batch):
        finish(b)

    @pl.when(me < n_seq - 1)
    def _():
        for halo in halos:
            halo.wait_send()

    g_copy.wait_send()

    def drain(i, _):
        s_copy(2 * i).wait_send()
        t_copy(i, core).wait_send()

        @pl.when(me + 2 < n_seq)
        def _():
            e_copy(i).wait_send()

        return 0

    lax.fori_loop(0, steps, drain, 0)
    for b in range(batch):
        for r in range(1, n_mp):
            sq_copy(b, r).wait_send()
            lax.fori_loop(0, pieces, lambda p, _, b=b, r=r: (p_copy(b, r, p).wait_send(), 0)[1], 0)


def body(
    x_inner,
    z_gate,
    b_input,
    c_input,
    dt_raw,
    doc_ids,
    conv_x,
    conv_b,
    conv_c,
    dt_bias,
    decay_rate,
    norm_gain,
    w_out,
):
    batch, length, channels = x_inner.shape
    heads = dt_raw.shape[2]
    n_state = b_input.shape[2]
    taps = conv_x.shape[0]
    n_mp = lax.axis_size("mp")
    width = w_out.shape[1] // n_mp
    aligned = width % LANES == 0
    piece = 2 * LANES if width % (2 * LANES) == 0 else width
    pieces = width // piece
    cw = 2 * LANES if channels % (2 * LANES) == 0 else LANES
    units = batch * channels // cw
    steps = units // 2
    weights = w_out
    if not aligned:
        weights = w_out.reshape(channels, n_mp, width).transpose(1, 0, 2)
    docs = jnp.broadcast_to(doc_ids.astype(F32)[:, None, :], (batch, 8, length))
    others = n_mp - 1
    dims = (batch, length, channels, heads, width, piece, aligned, n_mp)
    vmem = pl.BlockSpec(memory_space=pltpu.VMEM)
    hbm = pl.BlockSpec(memory_space=pl.ANY)
    dma = pltpu.SemaphoreType.DMA
    V = pltpu.VMEM
    return pl.pallas_call(
        functools.partial(kernel, dims),
        out_shape=jax.ShapeDtypeStruct((batch, length, width), BF16),
        in_specs=[vmem, hbm, vmem, vmem, vmem, vmem, vmem, vmem, vmem, vmem, vmem, vmem, hbm],
        out_specs=vmem,
        scratch_shapes=[
            V((batch, length, channels), BF16),
            V((n_mp * pieces, channels, piece), BF16),
            V((batch, EDGE, channels), BF16),
            V((batch, EDGE, n_state), BF16),
            V((batch, EDGE, n_state), BF16),
            V((batch, 8, length), F32),
            V((batch, taps - 1, length, cw), F32),
            V((batch, length, channels), BF16),
            V((batch, length, n_state), BF16),
            V((batch, n_state, length), BF16),
            V((batch, length, length), F32),
            V((batch, length, LANES), F32),
            V((batch, length, LANES), F32),
            V((batch, length, LANES), F32),
            V((batch, LANES, length), F32),
            V((2 * batch, length, LANES), F32),
            V((units, n_state, cw), BF16),
            V((steps, n_state, cw), BF16),
            V((units, 8, cw), F32),
            V((units, 8, cw), F32),
            V((steps, n_state, cw), BF16),
            V((steps, n_state, cw), BF16),
            V((steps, n_state, cw), BF16),
            V((units, n_state, cw), BF16),
            V((batch, length, channels), F32),
            V((length, channels), BF16),
            V((batch * others * pieces, length, piece), BF16),
            V((batch * others * pieces, length, piece), BF16),
            V((batch * pieces, length, piece), F32),
            V((batch, 8, length), F32),
            V((batch * others, 8, length), F32),
            dma,
            dma((n_mp * pieces,)),
            dma((4,)),
            dma((4,)),
            dma((steps,)),
            dma((steps,)),
            dma,
            dma,
            dma((steps,)),
            dma((steps,)),
            dma((steps,)),
            dma((steps,)),
            dma((batch * others * pieces,)),
            dma((batch * others * pieces,)),
            dma((batch * others,)),
            dma((batch * others,)),
        ],
        compiler_params=pltpu.CompilerParams(
            collective_id=0, has_side_effects=True, vmem_limit_bytes=62 * 1024 * 1024
        ),
        name="mixer",
    )(
        x_inner,
        z_gate,
        b_input,
        c_input,
        dt_raw,
        docs,
        conv_x,
        conv_b,
        conv_c,
        dt_bias[None, :],
        decay_rate[None, :],
        norm_gain[None, :],
        weights,
    )


def solution(mesh):
    placed = (
        P(None, "seq", "mp"),
        P(None, "seq", "mp"),
        P(None, "seq", None),
        P(None, "seq", None),
        P(None, "seq", "mp"),
        P(None, "seq"),
        P(None, "mp"),
        P(),
        P(),
        P("mp"),
        P("mp"),
        P("mp"),
        P("mp", None),
    )
    return jax.shard_map(
        body, mesh=mesh, in_specs=placed, out_specs=P(None, "seq", "mp"), check_vma=False
    )
```

```python
import functools

import jax
import jax.numpy as jnp
from jax import lax
from jax.experimental import pallas as pl
from jax.experimental.pallas import tpu as pltpu
from jax.sharding import PartitionSpec as P

EPSILON = 1e-05
LANES = 128
EDGE = 16
LOG2E = 1.4426950408889634
CAP = 80.0
MESH = pl.DeviceIdType.MESH
F32 = jnp.float32
BF16 = jnp.bfloat16


def silu(value):
    half = 0.5 * value
    return half + half * jnp.tanh(half)


def wide(value, width):
    return value if width == LANES else jnp.concatenate([value] * (width // LANES), axis=1)


def kernel(
    dims,
    x_hbm,
    z_hbm,
    b_ref,
    c_ref,
    dt_ref,
    doc_ref,
    wx_ref,
    wb_ref,
    wc_ref,
    bias_ref,
    rate_ref,
    gain_ref,
    w_hbm,
    out_ref,
    x_ref,
    z_ref,
    w_ref,
    hx_ref,
    hb_ref,
    hc_ref,
    hd_ref,
    same_ref,
    xc_ref,
    cc_ref,
    bt_ref,
    score_ref,
    col_ref,
    load_ref,
    entry_ref,
    row_ref,
    pad_ref,
    s_ref,
    r_ref,
    g_ref,
    gr_ref,
    e_ref,
    o_ref,
    t_ref,
    en_ref,
    inner_ref,
    factor_ref,
    gn_ref,
    p_ref,
    q_ref,
    own_ref,
    sq_ref,
    sqr_ref,
    x_sem,
    z_sem,
    w_sem,
    doc_send,
    doc_recv,
    halo_send,
    halo_recv,
    s_send,
    s_recv,
    g_send,
    g_recv,
    e_send,
    e_recv,
    t_send,
    t_recv,
    p_send,
    p_recv,
    sq_send,
    sq_recv,
):
    batch, length, channels, heads, width, piece, aligned, n_mp = dims
    inner_total = channels * n_mp
    head_dim = channels // heads
    cw = LANES
    per_tile = LANES // head_dim
    per_chunk = cw // head_dim
    chunks = channels // cw
    units = batch * chunks
    steps = units // 2
    pieces = width // piece
    n_seq = lax.axis_size("seq")
    me = lax.axis_index("seq")
    my = lax.axis_index("mp")
    core = lax.rem(me, 2)
    sibling = me + 1 - 2 * core

    def blocks(k):
        if aligned:
            return w_hbm.at[:, pl.ds(pl.multiple_of(k * piece, piece), piece)]
        return w_hbm.at[k]

    barrier = pltpu.get_barrier_semaphore()
    expected = jnp.int32(n_mp - 1)
    for distance in (-2, -1, 1, 2):
        there = me + distance
        valid = jnp.logical_and(there >= 0, there < n_seq)
        expected = expected + valid.astype(jnp.int32)

        @pl.when(valid)
        def _(there=there):
            pl.semaphore_signal(barrier, inc=1, device_id={"seq": there}, device_id_type=MESH)

    for r in range(1, n_mp):
        pl.semaphore_signal(
            barrier, inc=1, device_id={"mp": lax.rem(my + r, n_mp)}, device_id_type=MESH
        )
    z_copy = pltpu.make_async_copy(z_hbm, z_ref, z_sem)
    x_copies = [
        pltpu.make_async_copy(x_hbm.at[b], x_ref.at[b], x_sem.at[b]) for b in range(batch)
    ]
    for x_copy in x_copies:
        x_copy.start()

    def w_copy(k):
        return pltpu.make_async_copy(blocks(k), w_ref.at[k], w_sem.at[k])

    def w_start(k, _):
        w_copy(k).start()
        return 0

    pl.semaphore_wait(barrier, expected)

    def remote(src, dst, send, recv, **there):
        return pltpu.make_async_remote_copy(
            src_ref=src,
            dst_ref=dst,
            send_sem=send,
            recv_sem=recv,
            device_id=there,
            device_id_type=MESH,
        )

    right = lax.rem(me + 1, n_seq)
    last = pl.ds(length - EDGE, EDGE)
    halos = [
        [
            remote(b_ref.at[b, last], hb_ref.at[b], halo_send.at[b, 0], halo_recv.at[b, 0], seq=right),
            remote(c_ref.at[b, last], hc_ref.at[b], halo_send.at[b, 1], halo_recv.at[b, 1], seq=right),
            remote(x_hbm.at[b, last], hx_ref.at[b], halo_send.at[b, 2], halo_recv.at[b, 2], seq=right),
        ]
        for b in range(batch)
    ]
    doc_copy = remote(doc_ref, hd_ref, doc_send, doc_recv, seq=right)

    @pl.when(me < n_seq - 1)
    def _():
        doc_copy.start()
        for halo in halos:
            for copy in halo:
                copy.start()

    z_copy.start()
    lax.fori_loop(0, n_mp * pieces, w_start, 0)

    @pl.when(me == 0)
    def _():
        hd_ref[...] = jnp.full_like(hd_ref, -1)
        hb_ref[...] = jnp.zeros_like(hb_ref)
        hc_ref[...] = jnp.zeros_like(hc_ref)
        hx_ref[...] = jnp.zeros_like(hx_ref)

    @pl.when(me < 2)
    def _():
        e_ref[...] = jnp.zeros_like(e_ref)

    rows = lax.broadcasted_iota(jnp.int32, (length, length), 0)
    columns = lax.broadcasted_iota(jnp.int32, (length, length), 1)
    causal = rows >= columns
    triangle = jnp.where(causal, 1.0, 0.0).astype(F32)
    lane_ids = lax.broadcasted_iota(jnp.int32, (length, LANES), 1)

    for b in range(batch):
        row_ref[b] = jnp.zeros((LANES, length), F32)
        row_ref[b, 0:heads, :] = dt_ref[b]
        step = row_ref[b].T[:, 0:heads] + bias_ref[...]
        step = jnp.maximum(step, 0.0) + jnp.log1p(jnp.exp(-jnp.abs(step)))
        pad_ref[b] = jnp.zeros((length, LANES), F32)
        pad_ref[batch + b] = jnp.ones((length, LANES), F32)
        pad_ref[b, :, 0:heads] = -(step * rate_ref[...])
        pad_ref[batch + b, :, 0:heads] = step
        logs = jnp.dot(
            triangle, pad_ref[b], precision=lax.Precision.HIGHEST, preferred_element_type=F32
        )
        col_ref[b] = logs * LOG2E
        row_ref[b] = (logs * LOG2E - jnp.log(pad_ref[batch + b]) * LOG2E).T

    @pl.when(me > 0)
    def _():
        doc_copy.wait_recv()

    def conv(now, halo, weight, same):
        full = jnp.concatenate([halo.astype(F32), now.astype(F32)], axis=0)
        taps = weight.shape[0]
        weight = weight.astype(F32)
        total = full[EDGE:] * weight[taps - 1 : taps]
        for lag in range(1, taps):
            shifted = pltpu.roll(full, lag, 0)[EDGE:]
            total = total + shifted * same[lag - 1] * weight[taps - 1 - lag : taps - lag]
        return silu(total)

    def prepare(b):
        x_copies[b].wait()

        @pl.when(me > 0)
        def _():
            for copy in halos[b]:
                copy.wait_recv()

        doc_row = doc_ref[b : b + 1, :].astype(F32)
        doc_col = jnp.broadcast_to(doc_row, (LANES, length)).T
        old_col = jnp.broadcast_to(hd_ref[b : b + 1, :].astype(F32), (LANES, length)).T
        full = jnp.concatenate([old_col[length - EDGE :], doc_col], axis=0)
        for lag in range(1, wx_ref.shape[0]):
            mark = pltpu.roll(full, lag, 0)[EDGE:]
            same = jnp.where(mark == doc_col, 1.0, 0.0).astype(F32)
            same_ref[b, lag - 1] = wide(same, cw)
        sames = [same_ref[b, lag, :, 0:LANES] for lag in range(wx_ref.shape[0] - 1)]
        b_conv = conv(b_ref[b], hb_ref[b], wb_ref[...], sames).astype(BF16)
        c_conv = conv(c_ref[b], hc_ref[b], wc_ref[...], sames).astype(BF16)
        cc_ref[b] = c_conv
        bt = b_conv.astype(F32).T.astype(BF16)
        bt_ref[b] = bt
        scores = jnp.dot(c_conv, bt, preferred_element_type=F32)
        masked = jnp.logical_and(causal, wide(doc_col, length) == doc_row)
        score_ref[b] = jnp.where(masked, scores, 0.0)
        logs = col_ref[b]
        step = pad_ref[batch + b]
        keeps = doc_col == doc_col[length - 1 : length]
        load_ref[b] = jnp.where(keeps, jnp.exp2(logs[length - 1 : length] - logs) * step, 0.0)
        before = old_col[length - 1 : length]
        entry_ref[b] = jnp.where(doc_col == before, jnp.exp2(logs), 0.0)

    def place(u):
        b = u // chunks
        c = u - b * chunks
        return b, c, pl.ds(pl.multiple_of(c * cw, cw), cw)

    def turned(value, c):
        return pltpu.roll(value, lax.rem(LANES - c * per_chunk, LANES), 1)

    def expand(value):
        ids = lax.broadcasted_iota(jnp.int32, (value.shape[0], LANES), 1)
        parts = []
        for tile in range(cw // LANES):
            first = tile * per_tile
            part = value[:, first : first + 1]
            for more in range(1, per_tile):
                column = value[:, first + more : first + more + 1]
                part = jnp.where(ids < more * head_dim, part, column)
            parts.append(jnp.broadcast_to(part, (value.shape[0], LANES)))
        return jnp.concatenate(parts, axis=1) if len(parts) > 1 else parts[0]

    def s_copy(u):
        return remote(
            s_ref.at[u], r_ref.at[u // 2], s_send.at[u // 2], s_recv.at[u // 2], seq=sibling
        )

    def front(u, _):
        b, c, where = place(u)
        sames = [same_ref[b, lag] for lag in range(wx_ref.shape[0] - 1)]
        x_conv = conv(x_ref[b, :, where], hx_ref[b, :, where], wx_ref[:, where], sames)
        x_conv = x_conv.astype(BF16)
        xc_ref[b, :, where] = x_conv
        weights = expand(turned(load_ref[b], c))
        weighted = (x_conv.astype(F32) * weights).astype(BF16)
        s_ref[u] = jnp.dot(bt_ref[b], weighted, preferred_element_type=F32).astype(BF16)
        gate = expand(turned(entry_ref[b, length - 8 : length, :], c))
        g_ref[u] = jnp.broadcast_to(gate[7:8], (8, cw))

        @pl.when(lax.rem(u, 2) != core)
        def _():
            s_copy(u).start()

        return 0

    bounds = [((b * chunks + 1) // 2, ((b + 1) * chunks + 1) // 2) for b in range(batch)]

    def g_copy(b):
        lower, upper = bounds[b]
        own = pl.ds(2 * lower, 2 * (upper - lower))
        return remote(g_ref.at[own], gr_ref.at[own], g_send.at[b], g_recv.at[b], seq=sibling)

    def fronts(b):
        if chunks % 2 == 0:
            prepare(b)
        elif b == 0:
            for every in range(batch):
                prepare(every)
        lower, upper = bounds[b]
        lax.fori_loop(2 * lower, 2 * upper, front, 0)
        g_copy(b).start()

    ahead = lax.rem(me + 2, n_seq)

    def e_copy(i):
        return remote(o_ref.at[i], e_ref.at[i], e_send.at[i], e_recv.at[i], seq=ahead)

    def t_copy(i, owner):
        u = 2 * i + owner
        return remote(t_ref.at[i], en_ref.at[u], t_send.at[i], t_recv.at[i], seq=sibling)

    def inner_unit(u, _):
        b, c, where = place(u)
        turned_logs = turned(col_ref[b], c)
        scores = score_ref[b]
        for tile in range(cw // LANES):
            lanes = pl.ds(pl.multiple_of(c * cw + tile * LANES, LANES), LANES)
            xs = xc_ref[b, :, lanes]
            total = None
            for more in range(per_tile):
                head = tile * per_tile + more
                column = turned_logs[:, head : head + 1]
                row = row_ref[b, pl.ds(c * per_chunk + head, 1), :]
                mixing = scores * jnp.exp2(jnp.minimum(column - row, CAP))
                one = jnp.dot(mixing.astype(BF16), xs, preferred_element_type=F32)
                total = one if more == 0 else jnp.where(lane_ids < more * head_dim, total, one)
            opened = silu(z_ref[b, :, lanes].astype(F32))
            inner_ref[b, :, lanes] = total * opened
            factor_ref[b, :, lanes] = expand(turned(entry_ref[b], c)) * opened
        return 0

    def chain(i, _):
        u = 2 * i + core
        s_copy(2 * i).wait_recv()
        mine, theirs = s_ref[u].astype(F32), r_ref[i].astype(F32)
        my_gate, their_gate = g_ref[u, 0:1, :], gr_ref[u, 0:1, :]
        first = core == 0
        state_a = jnp.where(first, mine, theirs)
        state_b = jnp.where(first, theirs, mine)
        gate_a = jnp.where(first, my_gate, their_gate)
        gate_b = jnp.where(first, their_gate, my_gate)

        @pl.when(me >= 2)
        def _():
            e_copy(i).wait_recv()

        entering = e_ref[i].astype(F32)
        middle = gate_a * entering + state_a
        o_ref[i] = (gate_b * middle + state_b).astype(BF16)

        @pl.when(me + 2 < n_seq)
        def _():
            e_copy(i).start()

        t_ref[i] = jnp.where(first, middle, entering).astype(BF16)
        t_copy(i, core).start()
        en_ref[u] = jnp.where(first, entering, middle).astype(BF16)
        return 0

    def t_wait(i, _):
        t_copy(i, 1 - core).wait_recv()
        return 0

    def p_slot(b, r, p):
        return (b * (n_mp - 1) + r - 1) * pieces + p

    def p_copy(b, r, p):
        slot = p_slot(b, r, p)
        return remote(
            p_ref.at[slot],
            q_ref.at[slot],
            p_send.at[slot],
            p_recv.at[slot],
            mp=lax.rem(my + r, n_mp),
        )

    def sq_copy(b, r):
        slot = b * (n_mp - 1) + r - 1
        return remote(
            sq_ref.at[b],
            sqr_ref.at[slot],
            sq_send.at[slot],
            sq_recv.at[slot],
            mp=lax.rem(my + r, n_mp),
        )

    def tail(b):
        def gate_unit(c, squares):
            where = pl.ds(pl.multiple_of(c * cw, cw), cw)
            outer = jnp.dot(cc_ref[b], en_ref[b * chunks + c], preferred_element_type=F32)
            gated = inner_ref[b, :, where] + factor_ref[b, :, where] * outer
            gn_ref[:, where] = (gated * gain_ref[pl.ds(c, 1), :]).astype(BF16)
            square = gated * gated
            for tile in range(cw // LANES):
                squares = squares + square[:, tile * LANES : (tile + 1) * LANES]
            return squares

        squares = lax.fori_loop(0, chunks, gate_unit, jnp.zeros((length, LANES), F32))
        sq_ref[b] = jnp.broadcast_to(jnp.sum(squares.T, axis=0, keepdims=True), (8, length))
        for r in range(1, n_mp):

            def project(p, _, r=r):
                k = lax.rem(my + r, n_mp) * pieces + p
                value = jnp.dot(gn_ref[...], w_ref[k], preferred_element_type=F32)
                p_ref[p_slot(b, r, p)] = value.astype(BF16)
                p_copy(b, r, p).start()
                return 0

            sq_copy(b, r).start()
            lax.fori_loop(0, pieces, project, 0)

        def project_own(p, _):
            value = jnp.dot(gn_ref[...], w_ref[my * pieces + p], preferred_element_type=F32)
            own_ref[b * pieces + p] = value
            return 0

        lax.fori_loop(0, pieces, project_own, 0)

    def finish(b):
        total = sq_ref[b]
        for r in range(1, n_mp):
            sq_copy(b, r).wait_recv()
            total = total + sqr_ref[b * (n_mp - 1) + r - 1]
        scale = lax.rsqrt(total[0:1] / inner_total + EPSILON)
        scale = jnp.broadcast_to(scale, (LANES, length)).T[:, 0:1]
        for p in range(pieces):
            value = own_ref[b * pieces + p]
            for r in range(1, n_mp):
                p_copy(b, r, p).wait_recv()
                value = value + q_ref[p_slot(b, r, p)].astype(F32)
            out_ref[b, :, p * piece : (p + 1) * piece] = (value * scale).astype(BF16)

    def inners():
        z_copy.wait()
        lax.fori_loop(0, units, inner_unit, 0)

    def chains(b):
        lower, upper = bounds[b]
        g_copy(b).wait_recv()
        lax.fori_loop(lower, upper, chain, 0)

    def returns(b):
        lower, upper = bounds[b]
        lax.fori_loop(lower, upper, t_wait, 0)

    late = me >= n_seq // 2
    fronts(0)

    @pl.when(late)
    def _():
        for b in range(1, batch):
            fronts(b)
        inners()

    chains(0)

    @pl.when(jnp.logical_not(late))
    def _():
        for b in range(1, batch):
            fronts(b)
        for b in range(1, batch):
            chains(b)
        inners()

    lax.fori_loop(0, n_mp * pieces, lambda k, _: (w_copy(k).wait(), 0)[1], 0)
    for b in range(batch):
        if b > 0:

            @pl.when(late)
            def _(b=b):
                chains(b)

        returns(b)
        tail(b)
    for b in range(batch):
        finish(b)

    @pl.when(me < n_seq - 1)
    def _():
        doc_copy.wait_send()
        for halo in halos:
            for copy in halo:
                copy.wait_send()

    for b in range(batch):
        g_copy(b).wait_send()

    def drain(i, _):
        s_copy(2 * i).wait_send()
        t_copy(i, core).wait_send()

        @pl.when(me + 2 < n_seq)
        def _():
            e_copy(i).wait_send()

        return 0

    lax.fori_loop(0, steps, drain, 0)
    for b in range(batch):
        for r in range(1, n_mp):
            sq_copy(b, r).wait_send()
            lax.fori_loop(0, pieces, lambda p, _, b=b, r=r: (p_copy(b, r, p).wait_send(), 0)[1], 0)


def body(
    x_inner,
    z_gate,
    b_input,
    c_input,
    dt_raw,
    doc_ids,
    conv_x,
    conv_b,
    conv_c,
    dt_bias,
    decay_rate,
    norm_gain,
    w_out,
):
    batch, length, channels = x_inner.shape
    heads = dt_raw.shape[2]
    n_state = b_input.shape[2]
    taps = conv_x.shape[0]
    n_mp = lax.axis_size("mp")
    width = w_out.shape[1] // n_mp
    aligned = width % LANES == 0
    piece = 2 * LANES if width % (2 * LANES) == 0 else width
    pieces = width // piece
    cw = LANES
    units = batch * channels // cw
    steps = units // 2
    weights = w_out
    if not aligned:
        weights = w_out.reshape(channels, n_mp, width).transpose(1, 0, 2)
    others = n_mp - 1
    dims = (batch, length, channels, heads, width, piece, aligned, n_mp)
    vmem = pl.BlockSpec(memory_space=pltpu.VMEM)
    hbm = pl.BlockSpec(memory_space=pl.ANY)
    dma = pltpu.SemaphoreType.DMA
    V = pltpu.VMEM
    return pl.pallas_call(
        functools.partial(kernel, dims),
        out_shape=jax.ShapeDtypeStruct((batch, length, width), BF16),
        in_specs=[hbm, hbm, vmem, vmem, vmem, vmem, vmem, vmem, vmem, vmem, vmem, vmem, hbm],
        out_specs=vmem,
        scratch_shapes=[
            V((batch, length, channels), BF16),
            V((batch, length, channels), BF16),
            V((n_mp * pieces, channels, piece), BF16),
            V((batch, EDGE, channels), BF16),
            V((batch, EDGE, n_state), BF16),
            V((batch, EDGE, n_state), BF16),
            V((batch, length), jnp.int32),
            V((batch, taps - 1, length, cw), F32),
            V((batch, length, channels), BF16),
            V((batch, length, n_state), BF16),
            V((batch, n_state, length), BF16),
            V((batch, length, length), F32),
            V((batch, length, LANES), F32),
            V((batch, length, LANES), F32),
            V((batch, length, LANES), F32),
            V((batch, LANES, length), F32),
            V((2 * batch, length, LANES), F32),
            V((units, n_state, cw), BF16),
            V((steps, n_state, cw), BF16),
            V((units, 8, cw), F32),
            V((units, 8, cw), F32),
            V((steps, n_state, cw), BF16),
            V((steps, n_state, cw), BF16),
            V((steps, n_state, cw), BF16),
            V((units, n_state, cw), BF16),
            V((batch, length, channels), F32),
            V((batch, length, channels), F32),
            V((length, channels), BF16),
            V((batch * others * pieces, length, piece), BF16),
            V((batch * others * pieces, length, piece), BF16),
            V((batch * pieces, length, piece), F32),
            V((batch, 8, length), F32),
            V((batch * others, 8, length), F32),
            dma((batch,)),
            dma,
            dma((n_mp * pieces,)),
            dma,
            dma,
            dma((batch, 3)),
            dma((batch, 3)),
            dma((steps,)),
            dma((steps,)),
            dma((batch,)),
            dma((batch,)),
            dma((steps,)),
            dma((steps,)),
            dma((steps,)),
            dma((steps,)),
            dma((batch * others * pieces,)),
            dma((batch * others * pieces,)),
            dma((batch * others,)),
            dma((batch * others,)),
        ],
        compiler_params=pltpu.CompilerParams(
            collective_id=0, has_side_effects=True, vmem_limit_bytes=62 * 1024 * 1024
        ),
        name="mixer",
    )(
        x_inner,
        z_gate,
        b_input,
        c_input,
        jnp.swapaxes(dt_raw, 1, 2),
        doc_ids,
        conv_x,
        conv_b,
        conv_c,
        dt_bias[None, :],
        decay_rate[None, :],
        norm_gain.reshape(channels // cw, cw),
        weights,
    )


def solution(mesh):
    placed = (
        P(None, "seq", "mp"),
        P(None, "seq", "mp"),
        P(None, "seq", None),
        P(None, "seq", None),
        P(None, "seq", "mp"),
        P(None, "seq"),
        P(None, "mp"),
        P(),
        P(),
        P("mp"),
        P("mp"),
        P("mp"),
        P("mp", None),
    )
    return jax.shard_map(
        body, mesh=mesh, in_specs=placed, out_specs=P(None, "seq", "mp"), check_vma=False
    )
```

```python
import functools

import jax
import jax.numpy as jnp
from jax import lax
from jax.experimental import pallas as pl
from jax.experimental.pallas import tpu as pltpu
from jax.sharding import PartitionSpec as P

EPSILON = 1e-05
LANES = 128
EDGE = 16
LOG2E = 1.4426950408889634
CAP = 80.0
MESH = pl.DeviceIdType.MESH
F32 = jnp.float32
BF16 = jnp.bfloat16


def silu(value):
    half = 0.5 * value
    return half + half * jnp.tanh(half)


def wide(value, width):
    return value if width == LANES else jnp.concatenate([value] * (width // LANES), axis=1)


def kernel(
    dims,
    x_hbm,
    z_hbm,
    b_ref,
    c_ref,
    dt_ref,
    doc_ref,
    wx_ref,
    wb_ref,
    wc_ref,
    bias_ref,
    rate_ref,
    gain_ref,
    w_hbm,
    out_ref,
    x_ref,
    z_ref,
    w_ref,
    hx_ref,
    hb_ref,
    hc_ref,
    hd_ref,
    same_ref,
    xc_ref,
    cc_ref,
    bt_ref,
    score_ref,
    col_ref,
    load_ref,
    entry_ref,
    row_ref,
    pad_ref,
    s_ref,
    r_ref,
    g_ref,
    gr_ref,
    e_ref,
    o_ref,
    t_ref,
    en_ref,
    inner_ref,
    factor_ref,
    gn_ref,
    p_ref,
    q_ref,
    own_ref,
    sq_ref,
    sqr_ref,
    x_sem,
    z_sem,
    w_sem,
    doc_send,
    doc_recv,
    halo_send,
    halo_recv,
    s_send,
    s_recv,
    g_send,
    g_recv,
    e_send,
    e_recv,
    t_send,
    t_recv,
    p_send,
    p_recv,
    sq_send,
    sq_recv,
):
    batch, length, channels, heads, width, piece, aligned, n_mp = dims
    inner_total = channels * n_mp
    head_dim = channels // heads
    cw = LANES
    per_tile = LANES // head_dim
    per_chunk = cw // head_dim
    chunks = channels // cw
    units = batch * chunks
    steps = units // 2
    pieces = width // piece
    tiles = 4 if chunks % 4 == 0 else 2
    n_seq = lax.axis_size("seq")
    me = lax.axis_index("seq")
    my = lax.axis_index("mp")
    core = lax.rem(me, 2)
    sibling = me + 1 - 2 * core

    def blocks(k):
        if aligned:
            return w_hbm.at[:, pl.ds(pl.multiple_of(k * piece, piece), piece)]
        return w_hbm.at[k]

    barrier = pltpu.get_barrier_semaphore()
    expected = jnp.int32(n_mp - 1)
    for distance in (-2, -1, 1, 2):
        there = me + distance
        valid = jnp.logical_and(there >= 0, there < n_seq)
        expected = expected + valid.astype(jnp.int32)

        @pl.when(valid)
        def _(there=there):
            pl.semaphore_signal(barrier, inc=1, device_id={"seq": there}, device_id_type=MESH)

    for r in range(1, n_mp):
        pl.semaphore_signal(
            barrier, inc=1, device_id={"mp": lax.rem(my + r, n_mp)}, device_id_type=MESH
        )
    z_copy = pltpu.make_async_copy(z_hbm, z_ref, z_sem)
    x_copies = [
        pltpu.make_async_copy(x_hbm.at[b], x_ref.at[b], x_sem.at[b]) for b in range(batch)
    ]
    for x_copy in x_copies:
        x_copy.start()

    def w_copy(k):
        return pltpu.make_async_copy(blocks(k), w_ref.at[k], w_sem.at[k])

    def w_start(k, _):
        w_copy(k).start()
        return 0

    pl.semaphore_wait(barrier, expected)

    def remote(src, dst, send, recv, **there):
        return pltpu.make_async_remote_copy(
            src_ref=src,
            dst_ref=dst,
            send_sem=send,
            recv_sem=recv,
            device_id=there,
            device_id_type=MESH,
        )

    right = lax.rem(me + 1, n_seq)
    last = pl.ds(length - EDGE, EDGE)
    halos = [
        [
            remote(b_ref.at[b, last], hb_ref.at[b], halo_send.at[b, 0], halo_recv.at[b, 0], seq=right),
            remote(c_ref.at[b, last], hc_ref.at[b], halo_send.at[b, 1], halo_recv.at[b, 1], seq=right),
            remote(x_hbm.at[b, last], hx_ref.at[b], halo_send.at[b, 2], halo_recv.at[b, 2], seq=right),
        ]
        for b in range(batch)
    ]
    doc_copy = remote(doc_ref, hd_ref, doc_send, doc_recv, seq=right)

    @pl.when(me < n_seq - 1)
    def _():
        doc_copy.start()
        for halo in halos:
            for copy in halo:
                copy.start()

    z_copy.start()
    lax.fori_loop(0, n_mp * pieces, w_start, 0)

    @pl.when(me == 0)
    def _():
        hd_ref[...] = jnp.full_like(hd_ref, -1)
        hb_ref[...] = jnp.zeros_like(hb_ref)
        hc_ref[...] = jnp.zeros_like(hc_ref)
        hx_ref[...] = jnp.zeros_like(hx_ref)

    @pl.when(me < 2)
    def _():
        e_ref[...] = jnp.zeros_like(e_ref)

    rows = lax.broadcasted_iota(jnp.int32, (length, length), 0)
    columns = lax.broadcasted_iota(jnp.int32, (length, length), 1)
    causal = rows >= columns
    triangle = jnp.where(causal, 1.0, 0.0).astype(F32)
    lane_ids = lax.broadcasted_iota(jnp.int32, (length, LANES), 1)

    for b in range(batch):
        row_ref[b] = jnp.zeros((LANES, length), F32)
        row_ref[b, 0:heads, :] = dt_ref[b]
        step = row_ref[b].T[:, 0:heads] + bias_ref[...]
        step = jnp.maximum(step, 0.0) + jnp.log1p(jnp.exp(-jnp.abs(step)))
        pad_ref[b] = jnp.zeros((length, LANES), F32)
        pad_ref[batch + b] = jnp.ones((length, LANES), F32)
        pad_ref[b, :, 0:heads] = -(step * rate_ref[...])
        pad_ref[batch + b, :, 0:heads] = step
        logs = jnp.dot(
            triangle, pad_ref[b], precision=lax.Precision.HIGHEST, preferred_element_type=F32
        )
        col_ref[b] = logs * LOG2E
        row_ref[b] = (logs * LOG2E - jnp.log(pad_ref[batch + b]) * LOG2E).T

    @pl.when(me > 0)
    def _():
        doc_copy.wait_recv()

    def conv(now, halo, weight, same):
        full = jnp.concatenate([halo.astype(F32), now.astype(F32)], axis=0)
        taps = weight.shape[0]
        weight = weight.astype(F32)
        total = full[EDGE:] * weight[taps - 1 : taps]
        for lag in range(1, taps):
            shifted = pltpu.roll(full, lag, 0)[EDGE:]
            total = total + shifted * same[lag - 1] * weight[taps - 1 - lag : taps - lag]
        return silu(total)

    def prepare(b):
        x_copies[b].wait()

        @pl.when(me > 0)
        def _():
            for copy in halos[b]:
                copy.wait_recv()

        doc_row = doc_ref[b : b + 1, :].astype(F32)
        doc_col = jnp.broadcast_to(doc_row, (LANES, length)).T
        old_col = jnp.broadcast_to(hd_ref[b : b + 1, :].astype(F32), (LANES, length)).T
        full = jnp.concatenate([old_col[length - EDGE :], doc_col], axis=0)
        for lag in range(1, wx_ref.shape[0]):
            mark = pltpu.roll(full, lag, 0)[EDGE:]
            same = jnp.where(mark == doc_col, 1.0, 0.0).astype(F32)
            same_ref[b, lag - 1] = wide(same, cw)
        sames = [same_ref[b, lag, :, 0:LANES] for lag in range(wx_ref.shape[0] - 1)]
        b_conv = conv(b_ref[b], hb_ref[b], wb_ref[...], sames).astype(BF16)
        c_conv = conv(c_ref[b], hc_ref[b], wc_ref[...], sames).astype(BF16)
        cc_ref[b] = c_conv
        bt = b_conv.astype(F32).T.astype(BF16)
        bt_ref[b] = bt
        scores = jnp.dot(c_conv, bt, preferred_element_type=F32)
        masked = jnp.logical_and(causal, wide(doc_col, length) == doc_row)
        score_ref[b] = jnp.where(masked, scores, 0.0)
        logs = col_ref[b]
        step = pad_ref[batch + b]
        keeps = doc_col == doc_col[length - 1 : length]
        load_ref[b] = jnp.where(keeps, jnp.exp2(logs[length - 1 : length] - logs) * step, 0.0)
        before = old_col[length - 1 : length]
        entry_ref[b] = jnp.where(doc_col == before, jnp.exp2(logs), 0.0)

    def place(u):
        b = u // chunks
        c = u - b * chunks
        return b, c, pl.ds(pl.multiple_of(c * cw, cw), cw)

    def turned(value, c):
        return pltpu.roll(value, lax.rem(LANES - c * per_chunk, LANES), 1)

    def expand(value):
        ids = lax.broadcasted_iota(jnp.int32, (value.shape[0], LANES), 1)
        parts = []
        for tile in range(cw // LANES):
            first = tile * per_tile
            part = value[:, first : first + 1]
            for more in range(1, per_tile):
                column = value[:, first + more : first + more + 1]
                part = jnp.where(ids < more * head_dim, part, column)
            parts.append(jnp.broadcast_to(part, (value.shape[0], LANES)))
        return jnp.concatenate(parts, axis=1) if len(parts) > 1 else parts[0]

    def s_copy(u):
        return remote(
            s_ref.at[u], r_ref.at[u // 2], s_send.at[u // 2], s_recv.at[u // 2], seq=sibling
        )

    def front_unit(u):
        b, c, where = place(u)
        sames = [same_ref[b, lag] for lag in range(wx_ref.shape[0] - 1)]
        x_conv = conv(x_ref[b, :, where], hx_ref[b, :, where], wx_ref[:, where], sames)
        x_conv = x_conv.astype(BF16)
        xc_ref[b, :, where] = x_conv
        weights = expand(turned(load_ref[b], c))
        weighted = (x_conv.astype(F32) * weights).astype(BF16)
        s_ref[u] = jnp.dot(bt_ref[b], weighted, preferred_element_type=F32).astype(BF16)
        gate = expand(turned(entry_ref[b, length - 8 : length, :], c))
        g_ref[u] = jnp.broadcast_to(gate[7:8], (8, cw))

    def front(group, _):
        for k in range(tiles):
            front_unit(group * tiles + k)
        for k in range(0, tiles, 2):
            s_copy(group * tiles + k + 1 - core).start()
        return 0

    bounds = [((b * chunks + 1) // 2, ((b + 1) * chunks + 1) // 2) for b in range(batch)]

    def g_copy(b):
        lower, upper = bounds[b]
        own = pl.ds(2 * lower, 2 * (upper - lower))
        return remote(g_ref.at[own], gr_ref.at[own], g_send.at[b], g_recv.at[b], seq=sibling)

    def fronts(b):
        if chunks % 2 == 0:
            prepare(b)
        elif b == 0:
            for every in range(batch):
                prepare(every)
        lower, upper = bounds[b]
        lax.fori_loop(2 * lower // tiles, 2 * upper // tiles, front, 0)
        g_copy(b).start()

    ahead = lax.rem(me + 2, n_seq)

    def e_copy(i):
        return remote(o_ref.at[i], e_ref.at[i], e_send.at[i], e_recv.at[i], seq=ahead)

    def t_copy(i, owner):
        u = 2 * i + owner
        return remote(t_ref.at[i], en_ref.at[u], t_send.at[i], t_recv.at[i], seq=sibling)

    def inner_unit(u):
        b, c, where = place(u)
        turned_logs = turned(col_ref[b], c)
        cut = length // 2
        for tile in range(cw // LANES):
            lanes = pl.ds(pl.multiple_of(c * cw + tile * LANES, LANES), LANES)
            xs = xc_ref[b, :, lanes]
            upper_rows, lower_rows = None, None
            for more in range(per_tile):
                head = tile * per_tile + more
                column = turned_logs[:, head : head + 1]
                row = row_ref[b, pl.ds(c * per_chunk + head, 1), :]
                spread = jnp.exp2(jnp.minimum(column[:cut] - row[:, :cut], CAP))
                mixing = (score_ref[b, :cut, :cut] * spread).astype(BF16)
                one = jnp.dot(mixing, xs[:cut], preferred_element_type=F32)
                spread = jnp.exp2(jnp.minimum(column[cut:] - row, CAP))
                mixing = (score_ref[b, cut:, :] * spread).astype(BF16)
                two = jnp.dot(mixing, xs, preferred_element_type=F32)
                if more == 0:
                    upper_rows, lower_rows = one, two
                else:
                    chosen = lane_ids[:cut] < more * head_dim
                    upper_rows = jnp.where(chosen, upper_rows, one)
                    lower_rows = jnp.where(chosen, lower_rows, two)
            total = jnp.concatenate([upper_rows, lower_rows], axis=0)
            opened = silu(z_ref[b, :, lanes].astype(F32))
            inner_ref[b, :, lanes] = total * opened
            factor_ref[b, :, lanes] = expand(turned(entry_ref[b], c)) * opened

    def inner(group, _):
        for k in range(tiles):
            inner_unit(group * tiles + k)
        return 0

    def chain(i, _, fill=False):
        u = 2 * i + core
        s_copy(2 * i).wait_recv()
        mine, theirs = s_ref[u].astype(F32), r_ref[i].astype(F32)
        my_gate, their_gate = g_ref[u, 0:1, :], gr_ref[u, 0:1, :]
        first = core == 0
        state_a = jnp.where(first, mine, theirs)
        state_b = jnp.where(first, theirs, mine)
        gate_a = jnp.where(first, my_gate, their_gate)
        gate_b = jnp.where(first, their_gate, my_gate)

        @pl.when(me >= 2)
        def _():
            e_copy(i).wait_recv()

        entering = e_ref[i].astype(F32)
        middle = gate_a * entering + state_a
        o_ref[i] = (gate_b * middle + state_b).astype(BF16)

        @pl.when(me + 2 < n_seq)
        def _():
            e_copy(i).start()

        t_ref[i] = jnp.where(first, middle, entering).astype(BF16)
        t_copy(i, core).start()
        en_ref[u] = jnp.where(first, entering, middle).astype(BF16)
        if fill:
            inner_unit(2 * i)
            inner_unit(2 * i + 1)
        return 0

    def t_wait(i, _):
        t_copy(i, 1 - core).wait_recv()
        return 0

    def p_slot(b, r, p):
        return (b * (n_mp - 1) + r - 1) * pieces + p

    def p_copy(b, r, p):
        slot = p_slot(b, r, p)
        return remote(
            p_ref.at[slot],
            q_ref.at[slot],
            p_send.at[slot],
            p_recv.at[slot],
            mp=lax.rem(my + r, n_mp),
        )

    def sq_copy(b, r):
        slot = b * (n_mp - 1) + r - 1
        return remote(
            sq_ref.at[b],
            sqr_ref.at[slot],
            sq_send.at[slot],
            sq_recv.at[slot],
            mp=lax.rem(my + r, n_mp),
        )

    def tail(b):
        span = 4 if chunks % 4 == 0 else 1

        def gate_units(group, squares):
            for k in range(span):
                c = group * span + k
                where = pl.ds(pl.multiple_of(c * cw, cw), cw)
                outer = jnp.dot(cc_ref[b], en_ref[b * chunks + c], preferred_element_type=F32)
                gated = inner_ref[b, :, where] + factor_ref[b, :, where] * outer
                gn_ref[:, where] = (gated * gain_ref[pl.ds(c, 1), :]).astype(BF16)
                squares = squares + gated * gated
            return squares

        squares = jnp.zeros((length, LANES), F32)
        squares = lax.fori_loop(0, chunks // span, gate_units, squares)
        sq_ref[b] = jnp.broadcast_to(jnp.sum(squares.T, axis=0, keepdims=True), (8, length))
        for r in range(1, n_mp):

            def project(p, _, r=r):
                k = lax.rem(my + r, n_mp) * pieces + p
                value = jnp.dot(gn_ref[...], w_ref[k], preferred_element_type=F32)
                p_ref[p_slot(b, r, p)] = value.astype(BF16)
                p_copy(b, r, p).start()
                return 0

            sq_copy(b, r).start()
            lax.fori_loop(0, pieces, project, 0)

        def project_own(p, _):
            value = jnp.dot(gn_ref[...], w_ref[my * pieces + p], preferred_element_type=F32)
            own_ref[b * pieces + p] = value
            return 0

        lax.fori_loop(0, pieces, project_own, 0)

    def finish(b):
        total = sq_ref[b]
        for r in range(1, n_mp):
            sq_copy(b, r).wait_recv()
            total = total + sqr_ref[b * (n_mp - 1) + r - 1]
        scale = lax.rsqrt(total[0:1] / inner_total + EPSILON)
        scale = jnp.broadcast_to(scale, (LANES, length)).T[:, 0:1]
        for p in range(pieces):
            value = own_ref[b * pieces + p]
            for r in range(1, n_mp):
                p_copy(b, r, p).wait_recv()
                value = value + q_ref[p_slot(b, r, p)].astype(F32)
            out_ref[b, :, p * piece : (p + 1) * piece] = (value * scale).astype(BF16)

    def inners(lower, upper):
        lax.fori_loop(lower, upper, inner, 0)

    def chains(b, fill):
        lower, upper = bounds[b]
        g_copy(b).wait_recv()
        lax.fori_loop(lower, upper, functools.partial(chain, fill=fill), 0)

    def returns(b):
        lower, upper = bounds[b]
        lax.fori_loop(lower, upper, t_wait, 0)

    late = me >= n_seq // 2
    last = me >= 3 * n_seq // 4
    half, whole = 2 * bounds[0][1] // tiles, units // tiles
    ready = jnp.where(last, whole, jnp.where(late, half, 0))
    fronts(0)

    @pl.when(late)
    def _():
        for b in range(1, batch):
            fronts(b)

    z_copy.wait()

    @pl.when(late)
    def _():
        inners(0, ready)
        chains(0, False)

    @pl.when(jnp.logical_not(late))
    def _():
        chains(0, True)
        for b in range(1, batch):
            fronts(b)
        for b in range(1, batch):
            chains(b, True)

    lax.fori_loop(0, n_mp * pieces, lambda k, _: (w_copy(k).wait(), 0)[1], 0)
    for b in range(batch):
        if b > 0:

            @pl.when(late)
            def _(b=b):
                chains(b, False)
                inners(ready, whole)

        returns(b)
        tail(b)
    for b in range(batch):
        finish(b)

    @pl.when(me < n_seq - 1)
    def _():
        doc_copy.wait_send()
        for halo in halos:
            for copy in halo:
                copy.wait_send()

    for b in range(batch):
        g_copy(b).wait_send()

    def drain(i, _):
        s_copy(2 * i).wait_send()
        t_copy(i, core).wait_send()

        @pl.when(me + 2 < n_seq)
        def _():
            e_copy(i).wait_send()

        return 0

    lax.fori_loop(0, steps, drain, 0)
    for b in range(batch):
        for r in range(1, n_mp):
            sq_copy(b, r).wait_send()
            lax.fori_loop(0, pieces, lambda p, _, b=b, r=r: (p_copy(b, r, p).wait_send(), 0)[1], 0)


def body(
    x_inner,
    z_gate,
    b_input,
    c_input,
    dt_raw,
    doc_ids,
    conv_x,
    conv_b,
    conv_c,
    dt_bias,
    decay_rate,
    norm_gain,
    w_out,
):
    batch, length, channels = x_inner.shape
    heads = dt_raw.shape[2]
    n_state = b_input.shape[2]
    taps = conv_x.shape[0]
    n_mp = lax.axis_size("mp")
    width = w_out.shape[1] // n_mp
    aligned = width % LANES == 0
    piece = 2 * LANES if width % (2 * LANES) == 0 else width
    pieces = width // piece
    cw = LANES
    units = batch * channels // cw
    steps = units // 2
    weights = w_out
    if not aligned:
        weights = w_out.reshape(channels, n_mp, width).transpose(1, 0, 2)
    others = n_mp - 1
    dims = (batch, length, channels, heads, width, piece, aligned, n_mp)
    vmem = pl.BlockSpec(memory_space=pltpu.VMEM)
    hbm = pl.BlockSpec(memory_space=pl.ANY)
    dma = pltpu.SemaphoreType.DMA
    V = pltpu.VMEM
    return pl.pallas_call(
        functools.partial(kernel, dims),
        out_shape=jax.ShapeDtypeStruct((batch, length, width), BF16),
        in_specs=[hbm, hbm, vmem, vmem, vmem, vmem, vmem, vmem, vmem, vmem, vmem, vmem, hbm],
        out_specs=vmem,
        scratch_shapes=[
            V((batch, length, channels), BF16),
            V((batch, length, channels), BF16),
            V((n_mp * pieces, channels, piece), BF16),
            V((batch, EDGE, channels), BF16),
            V((batch, EDGE, n_state), BF16),
            V((batch, EDGE, n_state), BF16),
            V((batch, length), jnp.int32),
            V((batch, taps - 1, length, cw), F32),
            V((batch, length, channels), BF16),
            V((batch, length, n_state), BF16),
            V((batch, n_state, length), BF16),
            V((batch, length, length), F32),
            V((batch, length, LANES), F32),
            V((batch, length, LANES), F32),
            V((batch, length, LANES), F32),
            V((batch, LANES, length), F32),
            V((2 * batch, length, LANES), F32),
            V((units, n_state, cw), BF16),
            V((steps, n_state, cw), BF16),
            V((units, 8, cw), F32),
            V((units, 8, cw), F32),
            V((steps, n_state, cw), BF16),
            V((steps, n_state, cw), BF16),
            V((steps, n_state, cw), BF16),
            V((units, n_state, cw), BF16),
            V((batch, length, channels), F32),
            V((batch, length, channels), F32),
            V((length, channels), BF16),
            V((batch * others * pieces, length, piece), BF16),
            V((batch * others * pieces, length, piece), BF16),
            V((batch * pieces, length, piece), F32),
            V((batch, 8, length), F32),
            V((batch * others, 8, length), F32),
            dma((batch,)),
            dma,
            dma((n_mp * pieces,)),
            dma,
            dma,
            dma((batch, 3)),
            dma((batch, 3)),
            dma((steps,)),
            dma((steps,)),
            dma((batch,)),
            dma((batch,)),
            dma((steps,)),
            dma((steps,)),
            dma((steps,)),
            dma((steps,)),
            dma((batch * others * pieces,)),
            dma((batch * others * pieces,)),
            dma((batch * others,)),
            dma((batch * others,)),
        ],
        compiler_params=pltpu.CompilerParams(
            collective_id=0, has_side_effects=True, vmem_limit_bytes=62 * 1024 * 1024
        ),
        name="mixer",
    )(
        x_inner,
        z_gate,
        b_input,
        c_input,
        jnp.swapaxes(dt_raw, 1, 2),
        doc_ids,
        conv_x,
        conv_b,
        conv_c,
        dt_bias[None, :],
        decay_rate[None, :],
        norm_gain.reshape(channels // cw, cw),
        weights,
    )


def solution(mesh):
    placed = (
        P(None, "seq", "mp"),
        P(None, "seq", "mp"),
        P(None, "seq", None),
        P(None, "seq", None),
        P(None, "seq", "mp"),
        P(None, "seq"),
        P(None, "mp"),
        P(),
        P(),
        P("mp"),
        P("mp"),
        P("mp"),
        P("mp", None),
    )
    return jax.shard_map(
        body, mesh=mesh, in_specs=placed, out_specs=P(None, "seq", "mp"), check_vma=False
    )
```

```python
import functools

import jax
import jax.numpy as jnp
from jax import lax
from jax.experimental import pallas as pl
from jax.experimental.pallas import tpu as pltpu
from jax.sharding import PartitionSpec as P

EPSILON = 1e-05
LANES = 128
EDGE = 16
LOG2E = 1.4426950408889634
CAP = 80.0
MESH = pl.DeviceIdType.MESH
F32 = jnp.float32
BF16 = jnp.bfloat16


def silu(value):
    half = 0.5 * value
    return half + half * jnp.tanh(half)


def wide(value, width):
    return value if width == LANES else jnp.concatenate([value] * (width // LANES), axis=1)


def kernel(
    dims,
    x_hbm,
    z_hbm,
    b_ref,
    c_ref,
    dt_ref,
    doc_ref,
    wx_ref,
    wb_ref,
    wc_ref,
    bias_ref,
    rate_ref,
    gain_ref,
    w_hbm,
    out_ref,
    x_ref,
    z_ref,
    w_ref,
    hx_ref,
    hb_ref,
    hc_ref,
    hd_ref,
    same_ref,
    xc_ref,
    cc_ref,
    bt_ref,
    score_ref,
    col_ref,
    load_ref,
    entry_ref,
    row_ref,
    pad_ref,
    s_ref,
    r_ref,
    g_ref,
    gr_ref,
    e_ref,
    o_ref,
    t_ref,
    en_ref,
    inner_ref,
    factor_ref,
    gn_ref,
    p_ref,
    q_ref,
    own_ref,
    sq_ref,
    sqr_ref,
    x_sem,
    z_sem,
    w_sem,
    doc_send,
    doc_recv,
    halo_send,
    halo_recv,
    s_send,
    s_recv,
    g_send,
    g_recv,
    e_send,
    e_recv,
    t_send,
    t_recv,
    p_send,
    p_recv,
    sq_send,
    sq_recv,
):
    batch, length, channels, heads, width, piece, aligned, n_mp = dims
    inner_total = channels * n_mp
    head_dim = channels // heads
    cw = LANES
    per_tile = LANES // head_dim
    per_chunk = cw // head_dim
    chunks = channels // cw
    units = batch * chunks
    steps = units // 2
    pieces = width // piece
    tiles = 4 if chunks % 4 == 0 else 2
    n_seq = lax.axis_size("seq")
    me = lax.axis_index("seq")
    my = lax.axis_index("mp")
    core = lax.rem(me, 2)
    sibling = me + 1 - 2 * core

    def blocks(k):
        if aligned:
            return w_hbm.at[:, pl.ds(pl.multiple_of(k * piece, piece), piece)]
        return w_hbm.at[k]

    barrier = pltpu.get_barrier_semaphore()
    expected = jnp.int32(n_mp - 1)
    for distance in (-2, -1, 1, 2):
        there = me + distance
        valid = jnp.logical_and(there >= 0, there < n_seq)
        expected = expected + valid.astype(jnp.int32)

        @pl.when(valid)
        def _(there=there):
            pl.semaphore_signal(barrier, inc=1, device_id={"seq": there}, device_id_type=MESH)

    for r in range(1, n_mp):
        pl.semaphore_signal(
            barrier, inc=1, device_id={"mp": lax.rem(my + r, n_mp)}, device_id_type=MESH
        )
    z_copy = pltpu.make_async_copy(z_hbm, z_ref, z_sem)
    x_copies = [
        pltpu.make_async_copy(x_hbm.at[b], x_ref.at[b], x_sem.at[b]) for b in range(batch)
    ]
    for x_copy in x_copies:
        x_copy.start()

    def w_copy(k):
        return pltpu.make_async_copy(blocks(k), w_ref.at[k], w_sem.at[k])

    def w_start(k, _):
        w_copy(k).start()
        return 0

    pl.semaphore_wait(barrier, expected)

    def remote(src, dst, send, recv, **there):
        return pltpu.make_async_remote_copy(
            src_ref=src,
            dst_ref=dst,
            send_sem=send,
            recv_sem=recv,
            device_id=there,
            device_id_type=MESH,
        )

    right = lax.rem(me + 1, n_seq)
    last = pl.ds(length - EDGE, EDGE)
    halos = [
        [
            remote(b_ref.at[b, last], hb_ref.at[b], halo_send.at[b, 0], halo_recv.at[b, 0], seq=right),
            remote(c_ref.at[b, last], hc_ref.at[b], halo_send.at[b, 1], halo_recv.at[b, 1], seq=right),
            remote(x_hbm.at[b, last], hx_ref.at[b], halo_send.at[b, 2], halo_recv.at[b, 2], seq=right),
        ]
        for b in range(batch)
    ]
    doc_copy = remote(doc_ref, hd_ref, doc_send, doc_recv, seq=right)

    @pl.when(me < n_seq - 1)
    def _():
        doc_copy.start()
        for halo in halos:
            for copy in halo:
                copy.start()

    z_copy.start()
    lax.fori_loop(0, n_mp * pieces, w_start, 0)

    @pl.when(me == 0)
    def _():
        hd_ref[...] = jnp.full_like(hd_ref, -1)
        hb_ref[...] = jnp.zeros_like(hb_ref)
        hc_ref[...] = jnp.zeros_like(hc_ref)
        hx_ref[...] = jnp.zeros_like(hx_ref)

    @pl.when(me < 2)
    def _():
        e_ref[...] = jnp.zeros_like(e_ref)

    rows = lax.broadcasted_iota(jnp.int32, (length, length), 0)
    columns = lax.broadcasted_iota(jnp.int32, (length, length), 1)
    causal = rows >= columns
    triangle = jnp.where(causal, 1.0, 0.0).astype(F32)
    lane_ids = lax.broadcasted_iota(jnp.int32, (length, LANES), 1)

    for b in range(batch):
        row_ref[b] = jnp.zeros((LANES, length), F32)
        row_ref[b, 0:heads, :] = dt_ref[b]
        step = row_ref[b].T[:, 0:heads] + bias_ref[...]
        step = jnp.maximum(step, 0.0) + jnp.log1p(jnp.exp(-jnp.abs(step)))
        pad_ref[b] = jnp.zeros((length, LANES), F32)
        pad_ref[batch + b] = jnp.ones((length, LANES), F32)
        pad_ref[b, :, 0:heads] = -(step * rate_ref[...])
        pad_ref[batch + b, :, 0:heads] = step
        logs = jnp.dot(
            triangle, pad_ref[b], precision=lax.Precision.HIGHEST, preferred_element_type=F32
        )
        col_ref[b] = logs * LOG2E
        row_ref[b] = (logs * LOG2E - jnp.log(pad_ref[batch + b]) * LOG2E).T

    @pl.when(me > 0)
    def _():
        doc_copy.wait_recv()

    def conv(now, halo, weight, same):
        full = jnp.concatenate([halo.astype(F32), now.astype(F32)], axis=0)
        taps = weight.shape[0]
        weight = weight.astype(F32)
        total = full[EDGE:] * weight[taps - 1 : taps]
        for lag in range(1, taps):
            shifted = pltpu.roll(full, lag, 0)[EDGE:]
            total = total + shifted * same[lag - 1] * weight[taps - 1 - lag : taps - lag]
        return silu(total)

    def prepare(b):
        x_copies[b].wait()

        @pl.when(me > 0)
        def _():
            for copy in halos[b]:
                copy.wait_recv()

        doc_row = doc_ref[b : b + 1, :].astype(F32)
        doc_col = jnp.broadcast_to(doc_row, (LANES, length)).T
        old_col = jnp.broadcast_to(hd_ref[b : b + 1, :].astype(F32), (LANES, length)).T
        full = jnp.concatenate([old_col[length - EDGE :], doc_col], axis=0)
        for lag in range(1, wx_ref.shape[0]):
            mark = pltpu.roll(full, lag, 0)[EDGE:]
            same = jnp.where(mark == doc_col, 1.0, 0.0).astype(F32)
            same_ref[b, lag - 1] = wide(same, cw)
        sames = [same_ref[b, lag, :, 0:LANES] for lag in range(wx_ref.shape[0] - 1)]
        b_conv = conv(b_ref[b], hb_ref[b], wb_ref[...], sames).astype(BF16)
        c_conv = conv(c_ref[b], hc_ref[b], wc_ref[...], sames).astype(BF16)
        cc_ref[b] = c_conv
        bt = b_conv.astype(F32).T.astype(BF16)
        bt_ref[b] = bt
        scores = jnp.dot(c_conv, bt, preferred_element_type=F32)
        masked = jnp.logical_and(causal, wide(doc_col, length) == doc_row)
        score_ref[b] = jnp.where(masked, scores, 0.0)
        logs = col_ref[b]
        step = pad_ref[batch + b]
        keeps = doc_col == doc_col[length - 1 : length]
        load_ref[b] = jnp.where(keeps, jnp.exp2(logs[length - 1 : length] - logs) * step, 0.0)
        before = old_col[length - 1 : length]
        entry_ref[b] = jnp.where(doc_col == before, jnp.exp2(logs), 0.0)

    def place(u):
        b = u // chunks
        c = u - b * chunks
        return b, c, pl.ds(pl.multiple_of(c * cw, cw), cw)

    def turned(value, c):
        return pltpu.roll(value, lax.rem(LANES - c * per_chunk, LANES), 1)

    def expand(value):
        ids = lax.broadcasted_iota(jnp.int32, (value.shape[0], LANES), 1)
        parts = []
        for tile in range(cw // LANES):
            first = tile * per_tile
            part = value[:, first : first + 1]
            for more in range(1, per_tile):
                column = value[:, first + more : first + more + 1]
                part = jnp.where(ids < more * head_dim, part, column)
            parts.append(jnp.broadcast_to(part, (value.shape[0], LANES)))
        return jnp.concatenate(parts, axis=1) if len(parts) > 1 else parts[0]

    def s_copy(u):
        return remote(
            s_ref.at[u], r_ref.at[u // 2], s_send.at[u // 2], s_recv.at[u // 2], seq=sibling
        )

    def front_unit(u):
        b, c, where = place(u)
        sames = [same_ref[b, lag] for lag in range(wx_ref.shape[0] - 1)]
        x_conv = conv(x_ref[b, :, where], hx_ref[b, :, where], wx_ref[:, where], sames)
        x_conv = x_conv.astype(BF16)
        xc_ref[b, :, where] = x_conv
        weights = expand(turned(load_ref[b], c))
        weighted = (x_conv.astype(F32) * weights).astype(BF16)
        s_ref[u] = jnp.dot(bt_ref[b], weighted, preferred_element_type=F32).astype(BF16)
        gate = expand(turned(entry_ref[b, length - 8 : length, :], c))
        g_ref[u] = jnp.broadcast_to(gate[7:8], (8, cw))

    def front(group, _):
        for k in range(tiles):
            front_unit(group * tiles + k)
        for k in range(0, tiles, 2):
            s_copy(group * tiles + k + 1 - core).start()
        return 0

    bounds = [((b * chunks + 1) // 2, ((b + 1) * chunks + 1) // 2) for b in range(batch)]

    def g_copy(b):
        lower, upper = bounds[b]
        own = pl.ds(2 * lower, 2 * (upper - lower))
        return remote(g_ref.at[own], gr_ref.at[own], g_send.at[b], g_recv.at[b], seq=sibling)

    def fronts(b):
        if chunks % 2 == 0:
            prepare(b)
        elif b == 0:
            for every in range(batch):
                prepare(every)
        lower, upper = bounds[b]
        lax.fori_loop(2 * lower // tiles, 2 * upper // tiles, front, 0)
        g_copy(b).start()

    ahead = lax.rem(me + 2, n_seq)

    def e_copy(i):
        return remote(o_ref.at[i], e_ref.at[i], e_send.at[i], e_recv.at[i], seq=ahead)

    def t_copy(i, owner):
        u = 2 * i + owner
        return remote(t_ref.at[i], en_ref.at[u], t_send.at[i], t_recv.at[i], seq=sibling)

    def inner_unit(u):
        b, c, where = place(u)
        turned_logs = turned(col_ref[b], c)
        cut = length // 2
        for tile in range(cw // LANES):
            lanes = pl.ds(pl.multiple_of(c * cw + tile * LANES, LANES), LANES)
            xs = xc_ref[b, :, lanes]
            upper_rows, lower_rows = None, None
            for more in range(per_tile):
                head = tile * per_tile + more
                column = turned_logs[:, head : head + 1]
                row = row_ref[b, pl.ds(c * per_chunk + head, 1), :]
                spread = jnp.exp2(jnp.minimum(column[:cut] - row[:, :cut], CAP))
                mixing = (score_ref[b, :cut, :cut] * spread).astype(BF16)
                one = jnp.dot(mixing, xs[:cut], preferred_element_type=F32)
                spread = jnp.exp2(jnp.minimum(column[cut:] - row, CAP))
                mixing = (score_ref[b, cut:, :] * spread).astype(BF16)
                two = jnp.dot(mixing, xs, preferred_element_type=F32)
                if more == 0:
                    upper_rows, lower_rows = one, two
                else:
                    chosen = lane_ids[:cut] < more * head_dim
                    upper_rows = jnp.where(chosen, upper_rows, one)
                    lower_rows = jnp.where(chosen, lower_rows, two)
            total = jnp.concatenate([upper_rows, lower_rows], axis=0)
            opened = silu(z_ref[b, :, lanes].astype(F32))
            inner_ref[b, :, lanes] = total * opened
            factor_ref[b, :, lanes] = expand(turned(entry_ref[b], c)) * opened

    def inner(group, _):
        for k in range(tiles):
            inner_unit(group * tiles + k)
        return 0

    def chain(i, _, fill=None):
        u = 2 * i + core
        s_copy(2 * i).wait_recv()
        mine, theirs = s_ref[u].astype(F32), r_ref[i].astype(F32)
        my_gate, their_gate = g_ref[u, 0:1, :], gr_ref[u, 0:1, :]
        first = core == 0
        state_a = jnp.where(first, mine, theirs)
        state_b = jnp.where(first, theirs, mine)
        gate_a = jnp.where(first, my_gate, their_gate)
        gate_b = jnp.where(first, their_gate, my_gate)

        @pl.when(me >= 2)
        def _():
            e_copy(i).wait_recv()

        entering = e_ref[i].astype(F32)
        middle = gate_a * entering + state_a
        o_ref[i] = (gate_b * middle + state_b).astype(BF16)

        @pl.when(me + 2 < n_seq)
        def _():
            e_copy(i).start()

        t_ref[i] = jnp.where(first, middle, entering).astype(BF16)
        t_copy(i, core).start()
        en_ref[u] = jnp.where(first, entering, middle).astype(BF16)
        if fill is not None:

            @pl.when(2 * i >= fill)
            def _():
                inner_unit(2 * i)
                inner_unit(2 * i + 1)

        return 0

    def t_wait(i, _):
        t_copy(i, 1 - core).wait_recv()
        return 0

    def p_slot(b, r, p):
        return (b * (n_mp - 1) + r - 1) * pieces + p

    def p_copy(b, r, p):
        slot = p_slot(b, r, p)
        return remote(
            p_ref.at[slot],
            q_ref.at[slot],
            p_send.at[slot],
            p_recv.at[slot],
            mp=lax.rem(my + r, n_mp),
        )

    def sq_copy(b, r):
        slot = b * (n_mp - 1) + r - 1
        return remote(
            sq_ref.at[b],
            sqr_ref.at[slot],
            sq_send.at[slot],
            sq_recv.at[slot],
            mp=lax.rem(my + r, n_mp),
        )

    def tail(b):
        span = 4 if chunks % 4 == 0 else 1

        def gate_units(group, squares):
            for k in range(span):
                c = group * span + k
                where = pl.ds(pl.multiple_of(c * cw, cw), cw)
                outer = jnp.dot(cc_ref[b], en_ref[b * chunks + c], preferred_element_type=F32)
                gated = inner_ref[b, :, where] + factor_ref[b, :, where] * outer
                gn_ref[:, where] = (gated * gain_ref[pl.ds(c, 1), :]).astype(BF16)
                squares = squares + gated * gated
            return squares

        squares = jnp.zeros((length, LANES), F32)
        squares = lax.fori_loop(0, chunks // span, gate_units, squares)
        sq_ref[b] = jnp.broadcast_to(jnp.sum(squares.T, axis=0, keepdims=True), (8, length))
        for r in range(1, n_mp):

            def project(p, _, r=r):
                k = lax.rem(my + r, n_mp) * pieces + p
                value = jnp.dot(gn_ref[...], w_ref[k], preferred_element_type=F32)
                p_ref[p_slot(b, r, p)] = value.astype(BF16)
                p_copy(b, r, p).start()
                return 0

            sq_copy(b, r).start()
            lax.fori_loop(0, pieces, project, 0)

        def project_own(p, _):
            value = jnp.dot(gn_ref[...], w_ref[my * pieces + p], preferred_element_type=F32)
            own_ref[b * pieces + p] = value
            return 0

        lax.fori_loop(0, pieces, project_own, 0)

    def finish(b):
        total = sq_ref[b]
        for r in range(1, n_mp):
            sq_copy(b, r).wait_recv()
            total = total + sqr_ref[b * (n_mp - 1) + r - 1]
        scale = lax.rsqrt(total[0:1] / inner_total + EPSILON)
        scale = jnp.broadcast_to(scale, (LANES, length)).T[:, 0:1]
        for p in range(pieces):
            value = own_ref[b * pieces + p]
            for r in range(1, n_mp):
                p_copy(b, r, p).wait_recv()
                value = value + q_ref[p_slot(b, r, p)].astype(F32)
            out_ref[b, :, p * piece : (p + 1) * piece] = (value * scale).astype(BF16)

    def inners(lower, upper):
        lax.fori_loop(lower, upper, inner, 0)

    def chains(b, fill):
        lower, upper = bounds[b]
        g_copy(b).wait_recv()
        lax.fori_loop(lower, upper, functools.partial(chain, fill=fill), 0)

    def returns(b):
        lower, upper = bounds[b]
        lax.fori_loop(lower, upper, t_wait, 0)

    late = me >= n_seq // 2
    last = me >= 3 * n_seq // 4
    half, whole = 2 * bounds[0][1] // tiles, units // tiles
    more = half + (whole - half) // 2
    ready = jnp.where(last, more, jnp.where(late, half, 0))
    fronts(0)

    @pl.when(late)
    def _():
        for b in range(1, batch):
            fronts(b)

    z_copy.wait()

    @pl.when(late)
    def _():
        inners(0, ready)
        chains(0, None)

    @pl.when(jnp.logical_not(late))
    def _():
        chains(0, 0)
        for b in range(1, batch):
            fronts(b)
        for b in range(1, batch):
            chains(b, 0)

    lax.fori_loop(0, n_mp * pieces, lambda k, _: (w_copy(k).wait(), 0)[1], 0)
    for b in range(batch):
        if b > 0:

            @pl.when(late)
            def _(b=b):
                chains(b, ready * tiles)

        returns(b)
        tail(b)
    for b in range(batch):
        finish(b)

    @pl.when(me < n_seq - 1)
    def _():
        doc_copy.wait_send()
        for halo in halos:
            for copy in halo:
                copy.wait_send()

    for b in range(batch):
        g_copy(b).wait_send()

    def drain(i, _):
        s_copy(2 * i).wait_send()
        t_copy(i, core).wait_send()

        @pl.when(me + 2 < n_seq)
        def _():
            e_copy(i).wait_send()

        return 0

    lax.fori_loop(0, steps, drain, 0)
    for b in range(batch):
        for r in range(1, n_mp):
            sq_copy(b, r).wait_send()
            lax.fori_loop(0, pieces, lambda p, _, b=b, r=r: (p_copy(b, r, p).wait_send(), 0)[1], 0)


def body(
    x_inner,
    z_gate,
    b_input,
    c_input,
    dt_raw,
    doc_ids,
    conv_x,
    conv_b,
    conv_c,
    dt_bias,
    decay_rate,
    norm_gain,
    w_out,
):
    batch, length, channels = x_inner.shape
    heads = dt_raw.shape[2]
    n_state = b_input.shape[2]
    taps = conv_x.shape[0]
    n_mp = lax.axis_size("mp")
    width = w_out.shape[1] // n_mp
    aligned = width % LANES == 0
    piece = 2 * LANES if width % (2 * LANES) == 0 else width
    pieces = width // piece
    cw = LANES
    units = batch * channels // cw
    steps = units // 2
    weights = w_out
    if not aligned:
        weights = w_out.reshape(channels, n_mp, width).transpose(1, 0, 2)
    others = n_mp - 1
    dims = (batch, length, channels, heads, width, piece, aligned, n_mp)
    vmem = pl.BlockSpec(memory_space=pltpu.VMEM)
    hbm = pl.BlockSpec(memory_space=pl.ANY)
    dma = pltpu.SemaphoreType.DMA
    V = pltpu.VMEM
    return pl.pallas_call(
        functools.partial(kernel, dims),
        out_shape=jax.ShapeDtypeStruct((batch, length, width), BF16),
        in_specs=[hbm, hbm, vmem, vmem, vmem, vmem, vmem, vmem, vmem, vmem, vmem, vmem, hbm],
        out_specs=vmem,
        scratch_shapes=[
            V((batch, length, channels), BF16),
            V((batch, length, channels), BF16),
            V((n_mp * pieces, channels, piece), BF16),
            V((batch, EDGE, channels), BF16),
            V((batch, EDGE, n_state), BF16),
            V((batch, EDGE, n_state), BF16),
            V((batch, length), jnp.int32),
            V((batch, taps - 1, length, cw), F32),
            V((batch, length, channels), BF16),
            V((batch, length, n_state), BF16),
            V((batch, n_state, length), BF16),
            V((batch, length, length), F32),
            V((batch, length, LANES), F32),
            V((batch, length, LANES), F32),
            V((batch, length, LANES), F32),
            V((batch, LANES, length), F32),
            V((2 * batch, length, LANES), F32),
            V((units, n_state, cw), BF16),
            V((steps, n_state, cw), BF16),
            V((units, 8, cw), F32),
            V((units, 8, cw), F32),
            V((steps, n_state, cw), BF16),
            V((steps, n_state, cw), BF16),
            V((steps, n_state, cw), BF16),
            V((units, n_state, cw), BF16),
            V((batch, length, channels), F32),
            V((batch, length, channels), F32),
            V((length, channels), BF16),
            V((batch * others * pieces, length, piece), BF16),
            V((batch * others * pieces, length, piece), BF16),
            V((batch * pieces, length, piece), F32),
            V((batch, 8, length), F32),
            V((batch * others, 8, length), F32),
            dma((batch,)),
            dma,
            dma((n_mp * pieces,)),
            dma,
            dma,
            dma((batch, 3)),
            dma((batch, 3)),
            dma((steps,)),
            dma((steps,)),
            dma((batch,)),
            dma((batch,)),
            dma((steps,)),
            dma((steps,)),
            dma((steps,)),
            dma((steps,)),
            dma((batch * others * pieces,)),
            dma((batch * others * pieces,)),
            dma((batch * others,)),
            dma((batch * others,)),
        ],
        compiler_params=pltpu.CompilerParams(
            collective_id=0, has_side_effects=True, vmem_limit_bytes=62 * 1024 * 1024
        ),
        name="mixer",
    )(
        x_inner,
        z_gate,
        b_input,
        c_input,
        jnp.swapaxes(dt_raw, 1, 2),
        doc_ids,
        conv_x,
        conv_b,
        conv_c,
        dt_bias[None, :],
        decay_rate[None, :],
        norm_gain.reshape(channels // cw, cw),
        weights,
    )


def solution(mesh):
    placed = (
        P(None, "seq", "mp"),
        P(None, "seq", "mp"),
        P(None, "seq", None),
        P(None, "seq", None),
        P(None, "seq", "mp"),
        P(None, "seq"),
        P(None, "mp"),
        P(),
        P(),
        P("mp"),
        P("mp"),
        P("mp"),
        P("mp", None),
    )
    return jax.shard_map(
        body, mesh=mesh, in_specs=placed, out_specs=P(None, "seq", "mp"), check_vma=False
    )
```
